64 devices in a mesh: dp: 4 (over x, y), tp: 16 (over z, core).
Axes of the slice: x: 2, y: 2, z: 8, core: 2. Of those that a mesh axis runs over, the one named last changes fastest.
The devices are a block of a 4x4x8 slice.
Arguments:
- hidden: bfloat16 [2048, 7168], P(('dp', 'tp')), parts along dimension 0
- cache_lat: bfloat16 [2048, 128, 512], P(('dp', 'tp')), parts along dimension 0
- cache_rope: bfloat16 [2048, 128, 64], P(('dp', 'tp')), parts along dimension 0
- seq_lens: int32 [2048], P(('dp', 'tp')), parts along dimension 0
- attn_norm: bfloat16 [7168], replicated
- w_query: bfloat16 [7168, 12288], replicated
- w_kv_down: bfloat16 [7168, 576], replicated
- kv_norm: bfloat16 [512], replicated
- w_key_up: bfloat16 [512, 8192], replicated
- w_val_up: bfloat16 [512, 8192], replicated
- w_out: bfloat16 [8192, 7168], replicated
- mlp_norm: bfloat16 [7168], replicated
- w_gate: bfloat16 [7168, 18432], P(None, 'tp')
- w_up: bfloat16 [7168, 18432], P(None, 'tp')
- w_down: bfloat16 [18432, 7168], P('tp')
Outputs:
- output 1: bfloat16 [2048, 7168], P(('dp', 'tp')), parts along dimension 0
- output 2: bfloat16 [2048, 512], P(('dp', 'tp')), parts along dimension 0
- output 3: bfloat16 [2048, 64], P(('dp', 'tp')), parts along dimension 0
There are 4 independent parts. The reference program is written for one: setup_inputs(seed, part) draws one part's arguments, and reference() takes and returns one part's arrays. A program takes and returns all parts, laid end to end along the dimension named above; an argument that names none is the same for every part.
All inputs are finite; a program needn't handle non-finite values.
Results may differ from the reference program's by a relative error of at most 0.0117004.
Values are sent between devices in bfloat16 or wider.
A program may use at most 768 MiB of HBM per device.

```python
import jax
import jax.numpy as jnp
from jax import lax

HIDDEN = 7168
NUM_HEADS = 64
FFN_DIM = 18432
CACHE_LEN = 128
BATCH = 512
KV_LORA = 512
ROPE_DIM = 64
NOPE_DIM = 128
VAL_DIM = 128
EPS = 1e-6
ROPE_BASE = 10000.0
SCALE = (NOPE_DIM + ROPE_DIM) ** -0.5


def setup_inputs(seed: int = 0, part: int = 0) -> dict:
    part_key = jax.random.fold_in(jax.random.key(seed), part)
    part_keys = jax.random.split(part_key, 7)
    shared_keys = jax.random.split(jax.random.key(seed + 1), 11)
    hidden = jax.random.normal(part_keys[0], (BATCH, HIDDEN), jnp.float32).astype(jnp.bfloat16)
    seq_lens = jax.random.randint(part_keys[1], (BATCH,), 0, CACHE_LEN, jnp.int32)
    seq_lens = seq_lens.at[0].set(CACHE_LEN - 1).at[1].set(0)
    slot_scale = jnp.where(jnp.arange(CACHE_LEN)[None, :] < seq_lens[:, None], 1.0, 2.0)[:, :, None]
    slot_gain = jax.random.normal(part_keys[2], (BATCH, CACHE_LEN, 1), jnp.float32)
    lat_dir = jax.random.normal(part_keys[3], (BATCH, 1, KV_LORA), jnp.float32)
    rope_dir = jax.random.normal(part_keys[4], (BATCH, 1, ROPE_DIM), jnp.float32)
    lat_noise = 0.5 * jax.random.normal(part_keys[5], (BATCH, CACHE_LEN, KV_LORA), jnp.float32)
    rope_noise = 0.5 * jax.random.normal(part_keys[6], (BATCH, CACHE_LEN, ROPE_DIM), jnp.float32)
    cache_lat = (slot_scale * (slot_gain * lat_dir + lat_noise)).astype(jnp.bfloat16)
    cache_rope = (slot_scale * (slot_gain * rope_dir + rope_noise)).astype(jnp.bfloat16)

    def norm_gain(rand_key, width):
        return (1.0 + 0.3 * jax.random.normal(rand_key, (width,), jnp.float32)).astype(jnp.bfloat16)

    def weight(rand_key, dims, fan_in):
        return (jax.random.normal(rand_key, dims, jnp.float32) * fan_in ** -0.5).astype(jnp.bfloat16)

    return {
        'hidden': hidden,
        'cache_lat': cache_lat,
        'cache_rope': cache_rope,
        'seq_lens': seq_lens,
        'attn_norm': norm_gain(shared_keys[0], HIDDEN),
        'w_query': weight(shared_keys[1], (HIDDEN, NUM_HEADS * (NOPE_DIM + ROPE_DIM)), HIDDEN),
        'w_kv_down': weight(shared_keys[2], (HIDDEN, KV_LORA + ROPE_DIM), HIDDEN),
        'kv_norm': norm_gain(shared_keys[3], KV_LORA),
        'w_key_up': weight(shared_keys[4], (KV_LORA, NUM_HEADS * NOPE_DIM), NOPE_DIM),
        'w_val_up': weight(shared_keys[5], (KV_LORA, NUM_HEADS * VAL_DIM), KV_LORA),
        'w_out': weight(shared_keys[6], (NUM_HEADS * VAL_DIM, HIDDEN), NUM_HEADS * VAL_DIM),
        'mlp_norm': norm_gain(shared_keys[7], HIDDEN),
        'w_gate': weight(shared_keys[8], (HIDDEN, FFN_DIM), HIDDEN),
        'w_up': weight(shared_keys[9], (HIDDEN, FFN_DIM), HIDDEN),
        'w_down': weight(shared_keys[10], (FFN_DIM, HIDDEN), FFN_DIM),
    }


def rms_norm(vals, gain):
    vals32 = vals.astype(jnp.float32)
    inv_rms = lax.rsqrt(jnp.mean(vals32 * vals32, axis=-1, keepdims=True) + EPS)
    return (vals32 * inv_rms * gain.astype(jnp.float32)).astype(jnp.bfloat16)


def rotate(vals, cos_tab, sin_tab):
    half = vals.shape[-1] // 2
    first = vals[..., :half]
    second = vals[..., half:]
    return jnp.concatenate([first * cos_tab - second * sin_tab, second * cos_tab + first * sin_tab], axis=-1)


def rope_tables(seq_lens):
    inv_freq = ROPE_BASE ** (-jnp.arange(0, ROPE_DIM, 2, dtype=jnp.float32) / ROPE_DIM)
    angles = seq_lens.astype(jnp.float32)[:, None] * inv_freq[None, :]
    return jnp.cos(angles), jnp.sin(angles)


def attend_one(packed):
    q_lat, q_rot, lat_rows, rope_rows, length, lat_new, rope_new = packed
    scores = (jnp.dot(q_lat, lat_rows.T, preferred_element_type=jnp.float32) + jnp.dot(q_rot, rope_rows.T, preferred_element_type=jnp.float32)) * SCALE
    score_new = (jnp.dot(q_lat, lat_new, preferred_element_type=jnp.float32) + jnp.dot(q_rot, rope_new, preferred_element_type=jnp.float32)) * SCALE
    valid = jnp.arange(CACHE_LEN) < length
    scores = jnp.where(valid[None, :], scores, -jnp.inf)
    top = jnp.maximum(jnp.max(scores, axis=-1), score_new)
    expo = jnp.exp(scores - top[:, None])
    expo_new = jnp.exp(score_new - top)
    denom = jnp.sum(expo, axis=-1) + expo_new
    probs = (expo / denom[:, None]).astype(jnp.bfloat16)
    prob_new = (expo_new / denom).astype(jnp.bfloat16)
    lat_sum = jnp.dot(probs, lat_rows, preferred_element_type=jnp.float32) + prob_new.astype(jnp.float32)[:, None] * lat_new.astype(jnp.float32)[None, :]
    return lat_sum.astype(jnp.bfloat16)


def reference(hidden, cache_lat, cache_rope, seq_lens, attn_norm, w_query, w_kv_down, kv_norm, w_key_up, w_val_up, w_out, mlp_norm, w_gate, w_up, w_down):
    normed = rms_norm(hidden, attn_norm)
    query = jnp.dot(normed, w_query, preferred_element_type=jnp.float32).astype(jnp.bfloat16).reshape(BATCH, NUM_HEADS, NOPE_DIM + ROPE_DIM)
    kv_proj = jnp.dot(normed, w_kv_down, preferred_element_type=jnp.float32).astype(jnp.bfloat16)
    lat_new = rms_norm(kv_proj[:, :KV_LORA], kv_norm)
    cos_tab, sin_tab = rope_tables(seq_lens)
    rope_new = rotate(kv_proj[:, KV_LORA:].astype(jnp.float32), cos_tab, sin_tab).astype(jnp.bfloat16)
    q_rot = rotate(query[:, :, NOPE_DIM:].astype(jnp.float32), cos_tab[:, None, :], sin_tab[:, None, :]).astype(jnp.bfloat16)
    key_up = w_key_up.reshape(KV_LORA, NUM_HEADS, NOPE_DIM).astype(jnp.float32)
    q_lat = jnp.einsum('bhn,khn->bhk', query[:, :, :NOPE_DIM].astype(jnp.float32), key_up).astype(jnp.bfloat16)
    lat_out = lax.map(attend_one, (q_lat, q_rot, cache_lat, cache_rope, seq_lens, lat_new, rope_new))
    val_up = w_val_up.reshape(KV_LORA, NUM_HEADS, VAL_DIM).astype(jnp.float32)
    head_out = jnp.einsum('bhk,khv->bhv', lat_out.astype(jnp.float32), val_up).astype(jnp.bfloat16).reshape(BATCH, NUM_HEADS * VAL_DIM)
    attn_out = jnp.dot(head_out, w_out, preferred_element_type=jnp.float32)
    resid = (hidden.astype(jnp.float32) + attn_out).astype(jnp.bfloat16)
    mlp_in = rms_norm(resid, mlp_norm)
    gate_proj = jnp.dot(mlp_in, w_gate, preferred_element_type=jnp.float32)
    up_proj = jnp.dot(mlp_in, w_up, preferred_element_type=jnp.float32)
    act = (jax.nn.silu(gate_proj) * up_proj).astype(jnp.bfloat16)
    mlp_out = jnp.dot(act, w_down, preferred_element_type=jnp.float32)
    out_hidden = (resid.astype(jnp.float32) + mlp_out).astype(jnp.bfloat16)
    return (out_hidden, lat_new, rope_new)
```

```python
import functools

import jax
import jax.numpy as jnp
from jax import lax
from jax.experimental import pallas as pl
from jax.experimental.pallas import tpu as pltpu
from jax.sharding import PartitionSpec as P

EPS = 1e-6
ROPE_BASE = 10000.0
value_a7 = 512
ROPE_DIM = 64
NOPE_DIM = 128
SCALE = (NOPE_DIM + ROPE_DIM) ** -0.5


def rms_norm(vals, gain):
    vals32 = vals.astype(jnp.float32)
    inv_rms = lax.rsqrt(jnp.mean(vals32 * vals32, axis=-1, keepdims=True) + EPS)
    return (vals32 * inv_rms * gain.astype(jnp.float32)).astype(jnp.bfloat16)


def rotate(vals, cos_tab, sin_tab):
    half = vals.shape[-1] // 2
    first = vals[..., :half]
    second = vals[..., half:]
    return jnp.concatenate([first * cos_tab - second * sin_tab, second * cos_tab + first * sin_tab], axis=-1)


def rope_tables(seq_lens):
    inv_freq = ROPE_BASE ** (-jnp.arange(0, ROPE_DIM, 2, dtype=jnp.float32) / ROPE_DIM)
    angles = seq_lens.astype(jnp.float32)[:, None] * inv_freq[None, :]
    return jnp.cos(angles), jnp.sin(angles)


def attention_block(hidden, cache_lat, cache_rope, seq_lens, attn_norm, w_query, w_kv_down, kv_norm, w_key_up, w_val_up):
    rows = hidden.shape[0]
    heads = w_key_up.shape[1] // NOPE_DIM
    normed = rms_norm(hidden, attn_norm)
    query = jnp.dot(normed, w_query, preferred_element_type=jnp.float32).astype(jnp.bfloat16).reshape(rows, heads, NOPE_DIM + ROPE_DIM)
    kv_proj = jnp.dot(normed, w_kv_down, preferred_element_type=jnp.float32).astype(jnp.bfloat16)
    lat_new = rms_norm(kv_proj[:, :value_a7], kv_norm)
    cos_tab, sin_tab = rope_tables(seq_lens)
    rope_new = rotate(kv_proj[:, value_a7:].astype(jnp.float32), cos_tab, sin_tab).astype(jnp.bfloat16)
    q_rot = rotate(query[:, :, NOPE_DIM:].astype(jnp.float32), cos_tab[:, None, :], sin_tab[:, None, :]).astype(jnp.bfloat16)
    key_up = w_key_up.reshape(value_a7, heads, NOPE_DIM)
    q_lat = jnp.einsum('bhn,khn->bhk', query[:, :, :NOPE_DIM], key_up, preferred_element_type=jnp.float32).astype(jnp.bfloat16)
    scores = (jnp.einsum('bhk,bsk->bhs', q_lat, cache_lat, preferred_element_type=jnp.float32) + jnp.einsum('bhr,bsr->bhs', q_rot, cache_rope, preferred_element_type=jnp.float32)) * SCALE
    score_new = (jnp.einsum('bhk,bk->bh', q_lat, lat_new, preferred_element_type=jnp.float32) + jnp.einsum('bhr,br->bh', q_rot, rope_new, preferred_element_type=jnp.float32)) * SCALE
    slots = cache_lat.shape[1]
    valid = jnp.arange(slots)[None, None, :] < seq_lens[:, None, None]
    scores = jnp.where(valid, scores, -jnp.inf)
    top = jnp.maximum(jnp.max(scores, axis=-1), score_new)
    expo = jnp.exp(scores - top[..., None])
    expo_new = jnp.exp(score_new - top)
    denom = jnp.sum(expo, axis=-1) + expo_new
    probs = (expo / denom[..., None]).astype(jnp.bfloat16)
    prob_new = (expo_new / denom).astype(jnp.bfloat16)
    lat_sum = jnp.einsum('bhs,bsk->bhk', probs, cache_lat, preferred_element_type=jnp.float32) + prob_new.astype(jnp.float32)[..., None] * lat_new.astype(jnp.float32)[:, None, :]
    lat_out = lat_sum.astype(jnp.bfloat16)
    val_up = w_val_up.reshape(value_a7, heads, -1)
    head_out = jnp.einsum('bhk,khv->bhv', lat_out, val_up, preferred_element_type=jnp.float32).astype(jnp.bfloat16).reshape(rows, -1)
    return head_out, lat_new, rope_new

MESH = pl.DeviceIdType.MESH
GATHER_LAG = 1
SCATTER_LAG = 1


def tail_kernel(n, tile, sub, o_ref, x_ref, gain_ref, wo_hbm, wg_hbm, wu_hbm, wd_hbm, out_ref,
                o_all, x_half, gain_s, wo_buf, wgu_buf, x1_all, xg, acc, ssq, act_all, wd_all, part,
                stage_up, stage_dn, ring_up, ring_dn, stage_out,
                pre_send, pre_recv, wo_sem, wgu_sem, wd_sem, wdp_send, wdp_recv,
                g_send, g_recv, p_send, p_recv, a_send, a_recv, r_send, r_recv, f_send, f_recv):
    f32, bf16 = jnp.float32, jnp.bfloat16
    rows, width = x_ref.shape
    half = width // 2
    tiles = half // tile
    subs = tile // sub
    ffn = wg_hbm.shape[1]
    chips = n // 2
    reach_max = chips // 2
    chip_rows = 2 * rows
    depth = part.shape[0]

    me = lax.axis_index('tp')
    core = lax.rem(me, 2)
    chip = lax.div(me, 2)
    other = 1 - core
    partner = me + 1 - 2 * core
    upper = lax.rem(me + 2, n)
    lower = lax.rem(me + n - 2, n)
    mine = pl.multiple_of(core * half, 128)
    theirs = pl.multiple_of(other * half, 128)

    def remote(src, dst, send_sem, recv_sem, dev):
        return pltpu.make_async_remote_copy(src_ref=src, dst_ref=dst, send_sem=send_sem, recv_sem=recv_sem, device_id={'tp': dev}, device_id_type=MESH)

    def wo_copy(i):
        slot = lax.rem(i, 2)
        return pltpu.make_async_copy(wo_hbm.at[:, pl.ds(pl.multiple_of(mine + i * sub, 128), sub)], wo_buf.at[slot], wo_sem.at[slot])

    def wgu_copies(t):
        slot = lax.rem(t, 2)
        out = []
        for h in range(2):
            for k, src in enumerate((wg_hbm, wu_hbm)):
                out.append(pltpu.make_async_copy(src.at[pl.ds(pl.multiple_of(h * half + t * tile, 128), tile), :], wgu_buf.at[slot, pl.ds(h * tile, tile), pl.ds(k * ffn, ffn)], wgu_sem.at[slot, 2 * h + k]))
        return out

    def wd_copy(t):
        return pltpu.make_async_copy(wd_hbm.at[:, pl.ds(pl.multiple_of(mine + t * tile, 128), tile)], wd_all.at[t, pl.ds(pl.multiple_of(core * ffn, 128), ffn), :], wd_sem.at[t])

    def wd_push(t):
        return remote(wd_hbm.at[:, pl.ds(pl.multiple_of(theirs + t * tile, 128), tile)], wd_all.at[t, pl.ds(pl.multiple_of(core * ffn, 128), ffn), :], wdp_send.at[t], wdp_recv.at[t], partner)

    def wd_arrival(t):
        return remote(wd_hbm.at[:, pl.ds(0, tile)], wd_all.at[t, pl.ds(pl.multiple_of(other * ffn, 128), ffn), :], wdp_send.at[t], wdp_recv.at[t], partner)

    wo_copy(0).start()
    wo_copy(1).start()

    barrier = pltpu.get_barrier_semaphore()
    for dev in (partner, upper, lower):
        pl.semaphore_signal(barrier, inc=1, device_id={'tp': dev}, device_id_type=MESH)
    pl.semaphore_wait(barrier, 3)

    my_rows = pl.ds(pl.multiple_of(core * rows, rows), rows)
    their_rows = pl.ds(pl.multiple_of(other * rows, rows), rows)
    o_push = remote(o_ref, o_all.at[my_rows, :], pre_send.at[0], pre_recv.at[0], partner)
    x_push = remote(x_ref.at[:, pl.ds(theirs, half)], x_half.at[my_rows, :], pre_send.at[1], pre_recv.at[1], partner)
    o_push.start()
    x_push.start()
    o_all[my_rows, :] = o_ref[...]
    x_half[my_rows, :] = x_ref[:, pl.ds(mine, half)]
    gain = gain_ref[...].astype(f32)
    gain_top = jnp.maximum(jnp.max(jnp.abs(gain), axis=1, keepdims=True), 1e-30)
    gain_s[...] = gain / gain_top
    acc[...] = jnp.zeros_like(acc)
    ssq[...] = jnp.zeros_like(ssq)
    remote(o_ref, o_all.at[their_rows, :], pre_send.at[0], pre_recv.at[0], partner).wait_recv()
    remote(x_ref.at[:, pl.ds(theirs, half)], x_half.at[their_rows, :], pre_send.at[1], pre_recv.at[1], partner).wait_recv()

    def reach(t, d):
        first = reach_max - lax.rem(t, 2)
        return first if d == 0 else chips - 1 - first

    def origin(h, d):
        return lax.rem(chip + chips - h, chips) if d == 0 else lax.rem(chip + h, chips)

    def block(t, src):
        return x1_all.at[core * tiles + t, pl.ds(pl.multiple_of(src * chip_rows, chip_rows), chip_rows), :]

    def ring_copy(t, src, hop, d):
        return remote(block(t, src), block(t, src), g_send.at[d, t, hop - 1], g_recv.at[d, t, hop - 1], upper if d == 0 else lower)

    def pair_copy(t, src):
        return remote(block(t, src), block(t, src), p_send.at[t], p_recv.at[t], partner)

    def produce(t):
        for q in range(subs):
            i = t * subs + q
            slot = lax.rem(i, 2)
            wo_copy(i).wait()
            prod = jnp.dot(o_all[...], wo_buf[slot], preferred_element_type=f32)
            x1 = (x_half[:, pl.ds(pl.multiple_of(i * sub, 128), sub)].astype(f32) + prod).astype(bf16)
            x1_all[core * tiles + t, pl.ds(pl.multiple_of(chip * chip_rows, chip_rows), chip_rows), pl.ds(q * sub, sub)] = x1

            @pl.when(i + 2 < tiles * subs)
            def _():
                wo_copy(i + 2).start()
        for d in range(2):
            ring_copy(t, chip, 1, d).start()
        pair_copy(t, chip).start()

    def forward(t, h):
        for d in range(2):
            @pl.when(h <= reach(t, d))
            def _():
                src = origin(h, d)
                ring_copy(t, src, h, d).wait_recv()

                @pl.when(h < reach(t, d))
                def _():
                    ring_copy(t, src, h + 1, d).start()
                pair_copy(t, src).start()

    def consume(t):
        slot = lax.rem(t, 2)
        whole = x1_all.at[other * tiles + t]
        remote(whole, whole, p_send.at[t], p_recv.at[t], partner).wait_recv()
        for h in range(2):
            @pl.loop(0, chips)
            def _(b):
                rs = pl.ds(pl.multiple_of(b * chip_rows, chip_rows), chip_rows)
                vals = x1_all[h * tiles + t, rs, :].astype(f32)
                sq = vals * vals
                tot = sq[:, 0:128]
                for k in range(1, tile // 128):
                    tot += sq[:, k * 128:(k + 1) * 128]
                ssq[rs, :] += tot
                xg[rs, h * tile:(h + 1) * tile] = (vals * gain_s[:, pl.ds(pl.multiple_of(h * half + t * tile, 128), tile)]).astype(bf16)
        for copy in wgu_copies(t):
            copy.wait()

        @pl.loop(0, 2 * ffn // 256)
        def _(i):
            cs = pl.ds(pl.multiple_of(i * 256, 256), 256)
            acc[:, cs] += jnp.dot(xg[...], wgu_buf[slot, :, cs], preferred_element_type=f32)

    last_hop = GATHER_LAG * reach_max

    def gather_round(j, carry):
        @pl.when(j < tiles)
        def _():
            produce(j)
        for h in range(1, reach_max + 1):
            t = j - GATHER_LAG * h

            @pl.when((t >= 0) & (t < tiles))
            def _():
                forward(t, h)
        t_use = j - last_hop - 1

        @pl.when((t_use >= 0) & (t_use < tiles))
        def _():
            consume(t_use)
        t_next = j - last_hop + 1

        @pl.when((t_next >= 0) & (t_next < tiles))
        def _():
            for copy in wgu_copies(t_next):
                copy.start()

        @pl.when((t_next >= 0) & (t_next < tiles))
        def _():
            wd_copy(t_next).start()
            wd_push(t_next).start()
        return carry

    lax.fori_loop(0, tiles + last_hop + 1, gather_round, 0)

    act_mine = pl.ds(pl.multiple_of(core * ffn, 128), ffn)
    act_theirs = pl.ds(pl.multiple_of(other * ffn, 128), ffn)

    def act_copy(b):
        ref = act_all.at[pl.ds(pl.multiple_of(b * chip_rows, chip_rows), chip_rows), act_mine]
        return remote(ref, ref, a_send.at[b], a_recv.at[b], partner)

    def act_arrival(b):
        ref = act_all.at[pl.ds(pl.multiple_of(b * chip_rows, chip_rows), chip_rows), act_theirs]
        return remote(ref, ref, a_send.at[b], a_recv.at[b], partner)

    @pl.loop(0, chips)
    def _(b):
        rs = pl.ds(pl.multiple_of(b * chip_rows, chip_rows), chip_rows)
        inv = lax.rsqrt(jnp.sum(ssq[rs, :], axis=1, keepdims=True) / width + EPS)
        gate = acc[rs, 0:ffn] * inv * gain_top
        upv = acc[rs, ffn:2 * ffn] * inv * gain_top
        act_all[rs, act_mine] = (gate / (1.0 + jnp.exp(-gate)) * upv).astype(bf16)
        act_copy(b).start()

    @pl.loop(0, chips)
    def _(b):
        act_arrival(b).wait_recv()

    ring_bufs = (ring_up, ring_dn)
    stage_bufs = (stage_up, stage_dn)

    def rows_of(c):
        return pl.ds(pl.multiple_of(c * chip_rows, chip_rows), chip_rows)

    def sum_copy(t, s, d):
        src = stage_bufs[d].at[t] if s == 1 else ring_bufs[d].at[t, s - 2]
        return remote(src, ring_bufs[d].at[t, s - 1], r_send.at[d, t, s - 1], r_recv.at[d, t, s - 1], upper if d == 0 else lower)

    def target(t, s, d):
        ahead = reach(t, d) - s + 1
        return lax.rem(chip + ahead, chips) if d == 0 else lax.rem(chip + chips - ahead, chips)

    def out_copy(t):
        return remote(stage_out.at[t], out_ref.at[:, pl.ds(pl.multiple_of(mine + t * tile, 128), tile)], f_send.at[t], f_recv.at[t], partner)

    def out_arrival(t):
        return remote(stage_out.at[t], out_ref.at[:, pl.ds(pl.multiple_of(theirs + t * tile, 128), tile)], f_send.at[t], f_recv.at[t], partner)

    def finish(t):
        slot = lax.rem(t, depth)
        for d in range(2):
            for s in range(1, reach_max + 1):
                @pl.when(s == reach(t, d))
                def _():
                    sum_copy(t, s, d).wait_recv()

        def total(c):
            near = pl.ds(pl.multiple_of(c * rows, rows), rows)
            far = pl.ds(pl.multiple_of(chip * chip_rows + c * rows, rows), rows)
            val = part[slot, far, :]
            for d in range(2):
                val += ring_bufs[d][t, reach(t, d) - 1, near, :].astype(f32)
            return (x1_all[core * tiles + t, far, :].astype(f32) + val).astype(bf16)

        stage_out[t] = total(other)
        out_copy(t).start()
        out_ref[:, pl.ds(pl.multiple_of(mine + t * tile, 128), tile)] = total(core)

    def scatter_round(j, carry):
        @pl.when(j < tiles)
        def _():
            slot = lax.rem(j, depth)
            wd_copy(j).wait()
            wd_arrival(j).wait_recv()

            @pl.loop(0, tile // 256)
            def _(i):
                cs = pl.ds(pl.multiple_of(i * 256, 256), 256)
                part[slot, :, cs] = jnp.dot(act_all[...], wd_all[j, :, cs], preferred_element_type=f32)
            for d in range(2):
                stage_bufs[d][j] = part[slot, rows_of(target(j, 1, d)), :].astype(bf16)
                sum_copy(j, 1, d).start()
        for s in range(2, reach_max + 1):
            t = j - SCATTER_LAG * (s - 1)

            @pl.when((t >= 0) & (t < tiles))
            def _():
                for d in range(2):
                    @pl.when(s <= reach(t, d))
                    def _():
                        sum_copy(t, s - 1, d).wait_recv()
                        buf = ring_bufs[d]
                        own = part[lax.rem(t, depth), rows_of(target(t, s, d)), :]
                        buf[t, s - 2] = (buf[t, s - 2].astype(f32) + own).astype(bf16)
                        sum_copy(t, s, d).start()
        t_end = j - SCATTER_LAG * reach_max

        @pl.when((t_end >= 0) & (t_end < tiles))
        def _():
            finish(t_end)
        return carry

    lax.fori_loop(0, tiles + SCATTER_LAG * reach_max, scatter_round, 0)

    o_push.wait_send()
    x_push.wait_send()

    @pl.loop(0, chips)
    def _(b):
        act_copy(b).wait_send()

    @pl.loop(0, tiles)
    def _(t):
        out_arrival(t).wait_recv()
        out_copy(t).wait_send()
        wd_push(t).wait_send()
        whole = x1_all.at[core * tiles + t]
        remote(whole, whole, p_send.at[t], p_recv.at[t], partner).wait_send()
        for d in range(2):
            for h in range(1, reach_max + 1):
                @pl.when(h <= reach(t, d))
                def _():
                    ring_copy(t, chip, h, d).wait_send()
                    sum_copy(t, h, d).wait_send()


def fused_tail(n, head_out, hidden, mlp_norm, w_out, w_gate, w_up, w_down, tile=512, sub=256):
    bf16, f32 = jnp.bfloat16, jnp.float32
    rows, width = hidden.shape
    inner = head_out.shape[1]
    ffn = w_gate.shape[1]
    half = width // 2
    tiles = half // tile
    chips = n // 2
    reach = chips // 2
    group = rows * n
    depth = min(tiles, SCATTER_LAG * reach + 1)
    dma = pltpu.SemaphoreType.DMA
    vmem = pl.BlockSpec(memory_space=pltpu.VMEM)
    hbm = pl.BlockSpec(memory_space=pl.ANY)
    scratch = [
        pltpu.VMEM((2 * rows, inner), bf16),
        pltpu.VMEM((2 * rows, half), bf16),
        pltpu.VMEM((1, width), f32),
        pltpu.VMEM((2, inner, sub), bf16),
        pltpu.VMEM((2, 2 * tile, 2 * ffn), bf16),
        pltpu.VMEM((2 * tiles, group, tile), bf16),
        pltpu.VMEM((group, 2 * tile), bf16),
        pltpu.VMEM((group, 2 * ffn), f32),
        pltpu.VMEM((group, 128), f32),
        pltpu.VMEM((group, 2 * ffn), bf16),
        pltpu.VMEM((tiles, 2 * ffn, tile), bf16),
        pltpu.VMEM((depth, group, tile), f32),
        pltpu.VMEM((tiles, 2 * rows, tile), bf16),
        pltpu.VMEM((tiles, 2 * rows, tile), bf16),
        pltpu.VMEM((tiles, reach, 2 * rows, tile), bf16),
        pltpu.VMEM((tiles, reach, 2 * rows, tile), bf16),
        pltpu.VMEM((tiles, rows, tile), bf16),
        dma((2,)), dma((2,)), dma((2,)), dma((2, 4)), dma((tiles,)), dma((tiles,)), dma((tiles,)),
        dma((2, tiles, reach)), dma((2, tiles, reach)), dma((tiles,)), dma((tiles,)),
        dma((chips,)), dma((chips,)), dma((2, tiles, reach)), dma((2, tiles, reach)), dma((tiles,)), dma((tiles,)),
    ]
    return pl.pallas_call(
        functools.partial(tail_kernel, n, tile, sub),
        out_shape=jax.ShapeDtypeStruct((rows, width), bf16),
        in_specs=[vmem, vmem, vmem, hbm, hbm, hbm, hbm],
        out_specs=vmem,
        scratch_shapes=scratch,
        compiler_params=pltpu.CompilerParams(collective_id=0, has_side_effects=True, vmem_limit_bytes=67_043_328),
        name='tail',
    )(head_out, hidden, mlp_norm.reshape(1, width), w_out, w_gate, w_up, w_down)


def solution(mesh):
    rows_spec = P(('dp', 'tp'), None)
    cache_spec = P(('dp', 'tp'), None, None)
    whole = P()
    in_specs = (rows_spec, cache_spec, cache_spec, P(('dp', 'tp')), whole, whole, whole, whole, whole, whole, whole, whole, P(None, 'tp'), P(None, 'tp'), P('tp', None))
    out_specs = (rows_spec, rows_spec, rows_spec)

    def device_step(hidden, cache_lat, cache_rope, seq_lens, attn_norm, w_query, w_kv_down, kv_norm, w_key_up, w_val_up, w_out, mlp_norm, w_gate, w_up, w_down):
        head_out, lat_new, rope_new = attention_block(hidden, cache_lat, cache_rope, seq_lens, attn_norm, w_query, w_kv_down, kv_norm, w_key_up, w_val_up)
        out_hidden = fused_tail(mesh.shape['tp'], head_out, hidden, mlp_norm, w_out, w_gate, w_up, w_down)
        return out_hidden, lat_new, rope_new

    return jax.shard_map(device_step, mesh=mesh, in_specs=in_specs, out_specs=out_specs, check_vma=False)
```

```python
import functools

import jax
import jax.numpy as jnp
from jax import lax
from jax.experimental import pallas as pl
from jax.experimental.pallas import tpu as pltpu
from jax.sharding import PartitionSpec as P

EPS = 1e-6
ROPE_BASE = 10000.0
value_a7 = 512
ROPE_DIM = 64
NOPE_DIM = 128
SCALE = (NOPE_DIM + ROPE_DIM) ** -0.5


def rms_norm(vals, gain):
    vals32 = vals.astype(jnp.float32)
    inv_rms = lax.rsqrt(jnp.mean(vals32 * vals32, axis=-1, keepdims=True) + EPS)
    return (vals32 * inv_rms * gain.astype(jnp.float32)).astype(jnp.bfloat16)


def rotate(vals, cos_tab, sin_tab):
    half = vals.shape[-1] // 2
    first = vals[..., :half]
    second = vals[..., half:]
    return jnp.concatenate([first * cos_tab - second * sin_tab, second * cos_tab + first * sin_tab], axis=-1)


def rope_tables(seq_lens):
    inv_freq = ROPE_BASE ** (-jnp.arange(0, ROPE_DIM, 2, dtype=jnp.float32) / ROPE_DIM)
    angles = seq_lens.astype(jnp.float32)[:, None] * inv_freq[None, :]
    return jnp.cos(angles), jnp.sin(angles)


def attention_block(hidden, cache_lat, cache_rope, seq_lens, attn_norm, w_query, w_kv_down, kv_norm, w_key_up, w_val_up):
    rows = hidden.shape[0]
    heads = w_key_up.shape[1] // NOPE_DIM
    query, kv_proj = paired_query(hidden, attn_norm, w_query, w_kv_down)
    query = query.reshape(rows, heads, NOPE_DIM + ROPE_DIM)
    lat_new = rms_norm(kv_proj[:, :value_a7], kv_norm)
    cos_tab, sin_tab = rope_tables(seq_lens)
    rope_new = rotate(kv_proj[:, value_a7:].astype(jnp.float32), cos_tab, sin_tab).astype(jnp.bfloat16)
    q_rot = rotate(query[:, :, NOPE_DIM:].astype(jnp.float32), cos_tab[:, None, :], sin_tab[:, None, :]).astype(jnp.bfloat16)
    key_up = w_key_up.reshape(value_a7, heads, NOPE_DIM)
    q_lat = jnp.einsum('bhn,khn->bhk', query[:, :, :NOPE_DIM], key_up, preferred_element_type=jnp.float32).astype(jnp.bfloat16)
    scores = (jnp.einsum('bhk,bsk->bhs', q_lat, cache_lat, preferred_element_type=jnp.float32) + jnp.einsum('bhr,bsr->bhs', q_rot, cache_rope, preferred_element_type=jnp.float32)) * SCALE
    score_new = (jnp.einsum('bhk,bk->bh', q_lat, lat_new, preferred_element_type=jnp.float32) + jnp.einsum('bhr,br->bh', q_rot, rope_new, preferred_element_type=jnp.float32)) * SCALE
    slots = cache_lat.shape[1]
    valid = jnp.arange(slots)[None, None, :] < seq_lens[:, None, None]
    scores = jnp.where(valid, scores, -jnp.inf)
    top = jnp.maximum(jnp.max(scores, axis=-1), score_new)
    expo = jnp.exp(scores - top[..., None])
    expo_new = jnp.exp(score_new - top)
    denom = jnp.sum(expo, axis=-1) + expo_new
    probs = (expo / denom[..., None]).astype(jnp.bfloat16)
    prob_new = (expo_new / denom).astype(jnp.bfloat16)
    lat_sum = jnp.einsum('bhs,bsk->bhk', probs, cache_lat, preferred_element_type=jnp.float32) + prob_new.astype(jnp.float32)[..., None] * lat_new.astype(jnp.float32)[:, None, :]
    lat_out = lat_sum.astype(jnp.bfloat16)
    val_up = w_val_up.reshape(value_a7, heads, -1)
    head_out = jnp.einsum('bhk,khv->bhv', lat_out, val_up, preferred_element_type=jnp.float32).astype(jnp.bfloat16).reshape(rows, -1)
    return head_out, lat_new, rope_new

MESH = pl.DeviceIdType.MESH
GATHER_LAG = 2
SCATTER_LAG = 2

def query_kernel(sub, x_ref, gain_ref, wq_hbm, wkv_hbm, q_ref, kv_ref,
                 h_all, w_buf, wkv_buf, stage, kv_part, kv_stage, kv_in,
                 w_sem, wkv_sem, h_send, h_recv, k_send, k_recv, q_send, q_recv):
    f32, bf16 = jnp.float32, jnp.bfloat16
    rows, width = x_ref.shape
    half = width // 2
    q_half = wq_hbm.shape[1] // 2
    tiles = q_half // sub
    slots = w_buf.shape[0]
    me = lax.axis_index('tp')
    core = lax.rem(me, 2)
    other = 1 - core
    partner = me + 1 - 2 * core
    my_rows = pl.ds(pl.multiple_of(core * rows, rows), rows)
    their_rows = pl.ds(pl.multiple_of(other * rows, rows), rows)
    my_depth = pl.ds(pl.multiple_of(core * half, 128), half)

    def remote(src, dst, send_sem, recv_sem):
        return pltpu.make_async_remote_copy(src_ref=src, dst_ref=dst, send_sem=send_sem, recv_sem=recv_sem, device_id={'tp': partner}, device_id_type=MESH)

    def w_copy(i):
        slot = lax.rem(i, slots)
        return pltpu.make_async_copy(wq_hbm.at[:, pl.ds(pl.multiple_of(core * q_half + i * sub, 128), sub)], w_buf.at[slot], w_sem.at[slot])

    wkv_copy = pltpu.make_async_copy(wkv_hbm.at[my_depth, :], wkv_buf, wkv_sem.at[0])
    wkv_copy.start()
    for i in range(slots):
        w_copy(i).start()

    barrier = pltpu.get_barrier_semaphore()
    pl.semaphore_signal(barrier, inc=1, device_id={'tp': partner}, device_id_type=MESH)

    step = min(1024, width)
    tot = jnp.zeros((rows, 128), f32)
    for c in range(0, width, step):
        vals = x_ref[:, c:c + step].astype(f32)
        sq = vals * vals
        for k in range(0, step, 128):
            tot += sq[:, k:k + 128]
    inv = lax.rsqrt(jnp.sum(tot, axis=1, keepdims=True) / width + EPS)
    for c in range(0, width, step):
        vals = x_ref[:, c:c + step].astype(f32)
        h_all[my_rows, c:c + step] = (vals * inv * gain_ref[:, c:c + step].astype(f32)).astype(bf16)

    pl.semaphore_wait(barrier, 1)
    h_push = remote(h_all.at[my_rows, :], h_all.at[my_rows, :], h_send.at[0], h_recv.at[0])
    h_push.start()
    remote(h_all.at[their_rows, :], h_all.at[their_rows, :], h_send.at[0], h_recv.at[0]).wait_recv()

    wkv_copy.wait()
    kv_part[...] = jnp.dot(h_all[:, my_depth], wkv_buf[...], preferred_element_type=f32)
    kv_stage[...] = kv_part[their_rows, :]
    kv_push = remote(kv_stage, kv_in, k_send.at[0], k_recv.at[0])
    kv_push.start()

    def cols_of(c, i):
        return pl.ds(pl.multiple_of(c * q_half + i * sub, 128), sub)

    def q_copy(i):
        return remote(stage.at[i], q_ref.at[:, cols_of(core, i)], q_send.at[i], q_recv.at[i])

    @pl.loop(0, tiles)
    def _(i):
        slot = lax.rem(i, slots)
        w_copy(i).wait()
        prod = jnp.dot(h_all[...], w_buf[slot], preferred_element_type=f32).astype(bf16)

        @pl.when(i + slots < tiles)
        def _():
            w_copy(i + slots).start()
        low, high = prod[0:rows], prod[rows:2 * rows]
        first = core == 0
        q_ref[:, cols_of(core, i)] = jnp.where(first, low, high)
        stage[i] = jnp.where(first, high, low)
        q_copy(i).start()

    kv_push.wait_recv()
    kv_ref[...] = (kv_part[my_rows, :] + kv_in[...]).astype(bf16)
    h_push.wait_send()
    kv_push.wait_send()

    @pl.loop(0, tiles)
    def _(i):
        q_copy(i).wait_send()
        remote(stage.at[i], q_ref.at[:, cols_of(other, i)], q_send.at[i], q_recv.at[i]).wait_recv()


def paired_query(hidden, attn_norm, w_query, w_kv_down, sub=256):
    bf16, f32 = jnp.bfloat16, jnp.float32
    rows, width = hidden.shape
    q_cols = w_query.shape[1]
    kv_cols = w_kv_down.shape[1]
    tiles = q_cols // 2 // sub
    slots = min(8, tiles)
    dma = pltpu.SemaphoreType.DMA
    vmem = pl.BlockSpec(memory_space=pltpu.VMEM)
    hbm = pl.BlockSpec(memory_space=pl.ANY)
    scratch = [
        pltpu.VMEM((2 * rows, width), bf16),
        pltpu.VMEM((slots, width, sub), bf16),
        pltpu.VMEM((width // 2, kv_cols), bf16),
        pltpu.VMEM((tiles, rows, sub), bf16),
        pltpu.VMEM((2 * rows, kv_cols), f32),
        pltpu.VMEM((rows, kv_cols), f32),
        pltpu.VMEM((rows, kv_cols), f32),
        dma((slots,)), dma((1,)), dma((1,)), dma((1,)), dma((1,)), dma((1,)), dma((tiles,)), dma((tiles,)),
    ]
    return pl.pallas_call(
        functools.partial(query_kernel, sub),
        out_shape=(jax.ShapeDtypeStruct((rows, q_cols), bf16), jax.ShapeDtypeStruct((rows, kv_cols), bf16)),
        in_specs=[vmem, vmem, hbm, hbm],
        out_specs=(vmem, vmem),
        scratch_shapes=scratch,
        compiler_params=pltpu.CompilerParams(collective_id=1, has_side_effects=True, vmem_limit_bytes=60_000_000),
        name='query',
    )(hidden, attn_norm.reshape(1, width), w_query, w_kv_down)


def tail_kernel(n, tile, sub, o_ref, x_ref, gain_ref, wo_hbm, wg_hbm, wu_hbm, wd_hbm, out_ref,
                o_all, x_half, gain_s, wo_buf, wgu_buf, x1_all, xg, acc, ssq, act_all, wd_all, part,
                stage_up, stage_dn, ring_up, ring_dn, stage_out,
                pre_send, pre_recv, wo_sem, wgu_sem, wd_sem, wdp_send, wdp_recv,
                g_send, g_recv, p_send, p_recv, a_send, a_recv, r_send, r_recv, f_send, f_recv):
    f32, bf16 = jnp.float32, jnp.bfloat16
    rows, width = x_ref.shape
    half = width // 2
    tiles = half // tile
    subs = tile // sub
    ffn = wg_hbm.shape[1]
    chips = n // 2
    reach_max = chips // 2
    chip_rows = 2 * rows
    depth = part.shape[0]

    me = lax.axis_index('tp')
    core = lax.rem(me, 2)
    chip = lax.div(me, 2)
    other = 1 - core
    partner = me + 1 - 2 * core
    upper = lax.rem(me + 2, n)
    lower = lax.rem(me + n - 2, n)
    mine = pl.multiple_of(core * half, 128)
    theirs = pl.multiple_of(other * half, 128)

    def remote(src, dst, send_sem, recv_sem, dev):
        return pltpu.make_async_remote_copy(src_ref=src, dst_ref=dst, send_sem=send_sem, recv_sem=recv_sem, device_id={'tp': dev}, device_id_type=MESH)

    def wo_copy(i):
        slot = lax.rem(i, 2)
        return pltpu.make_async_copy(wo_hbm.at[:, pl.ds(pl.multiple_of(mine + i * sub, 128), sub)], wo_buf.at[slot], wo_sem.at[slot])

    def wgu_copies(t):
        slot = lax.rem(t, 2)
        out = []
        for h in range(2):
            for k, src in enumerate((wg_hbm, wu_hbm)):
                out.append(pltpu.make_async_copy(src.at[pl.ds(pl.multiple_of(h * half + t * tile, 128), tile), :], wgu_buf.at[slot, pl.ds(h * tile, tile), pl.ds(k * ffn, ffn)], wgu_sem.at[slot, 2 * h + k]))
        return out

    def wd_copy(t):
        return pltpu.make_async_copy(wd_hbm.at[:, pl.ds(pl.multiple_of(mine + t * tile, 128), tile)], wd_all.at[t, pl.ds(pl.multiple_of(core * ffn, 128), ffn), :], wd_sem.at[t])

    def wd_push(t):
        return remote(wd_hbm.at[:, pl.ds(pl.multiple_of(theirs + t * tile, 128), tile)], wd_all.at[t, pl.ds(pl.multiple_of(core * ffn, 128), ffn), :], wdp_send.at[t], wdp_recv.at[t], partner)

    def wd_arrival(t):
        return remote(wd_hbm.at[:, pl.ds(0, tile)], wd_all.at[t, pl.ds(pl.multiple_of(other * ffn, 128), ffn), :], wdp_send.at[t], wdp_recv.at[t], partner)

    wo_copy(0).start()
    wo_copy(1).start()

    barrier = pltpu.get_barrier_semaphore()
    for dev in (partner, upper, lower):
        pl.semaphore_signal(barrier, inc=1, device_id={'tp': dev}, device_id_type=MESH)
    pl.semaphore_wait(barrier, 3)

    my_rows = pl.ds(pl.multiple_of(core * rows, rows), rows)
    their_rows = pl.ds(pl.multiple_of(other * rows, rows), rows)
    o_push = remote(o_ref, o_all.at[my_rows, :], pre_send.at[0], pre_recv.at[0], partner)
    x_push = remote(x_ref.at[:, pl.ds(theirs, half)], x_half.at[my_rows, :], pre_send.at[1], pre_recv.at[1], partner)
    o_push.start()
    x_push.start()
    o_all[my_rows, :] = o_ref[...]
    x_half[my_rows, :] = x_ref[:, pl.ds(mine, half)]
    gain = gain_ref[...].astype(f32)
    gain_top = jnp.maximum(jnp.max(jnp.abs(gain), axis=1, keepdims=True), 1e-30)
    gain_s[...] = gain / gain_top
    acc[...] = jnp.zeros_like(acc)
    ssq[...] = jnp.zeros_like(ssq)
    remote(o_ref, o_all.at[their_rows, :], pre_send.at[0], pre_recv.at[0], partner).wait_recv()
    remote(x_ref.at[:, pl.ds(theirs, half)], x_half.at[their_rows, :], pre_send.at[1], pre_recv.at[1], partner).wait_recv()

    def reach(t, d):
        first = reach_max - lax.rem(t, 2)
        return first if d == 0 else chips - 1 - first

    def origin(h, d):
        return lax.rem(chip + chips - h, chips) if d == 0 else lax.rem(chip + h, chips)

    def block(t, src):
        return x1_all.at[core * tiles + t, pl.ds(pl.multiple_of(src * chip_rows, chip_rows), chip_rows), :]

    def ring_copy(t, src, hop, d):
        return remote(block(t, src), block(t, src), g_send.at[d, t, hop - 1], g_recv.at[d, t, hop - 1], upper if d == 0 else lower)

    def pair_copy(t, src):
        return remote(block(t, src), block(t, src), p_send.at[t], p_recv.at[t], partner)

    def produce(t):
        for q in range(subs):
            i = t * subs + q
            slot = lax.rem(i, 2)
            wo_copy(i).wait()
            prod = jnp.dot(o_all[...], wo_buf[slot], preferred_element_type=f32)
            x1 = (x_half[:, pl.ds(pl.multiple_of(i * sub, 128), sub)].astype(f32) + prod).astype(bf16)
            x1_all[core * tiles + t, pl.ds(pl.multiple_of(chip * chip_rows, chip_rows), chip_rows), pl.ds(q * sub, sub)] = x1

            @pl.when(i + 2 < tiles * subs)
            def _():
                wo_copy(i + 2).start()
        for d in range(2):
            ring_copy(t, chip, 1, d).start()
        pair_copy(t, chip).start()

    def forward(t, h):
        for d in range(2):
            @pl.when(h <= reach(t, d))
            def _():
                src = origin(h, d)
                ring_copy(t, src, h, d).wait_recv()

                @pl.when(h < reach(t, d))
                def _():
                    ring_copy(t, src, h + 1, d).start()
                pair_copy(t, src).start()

    def consume(t):
        slot = lax.rem(t, 2)
        whole = x1_all.at[other * tiles + t]
        remote(whole, whole, p_send.at[t], p_recv.at[t], partner).wait_recv()
        for h in range(2):
            @pl.loop(0, chips)
            def _(b):
                rs = pl.ds(pl.multiple_of(b * chip_rows, chip_rows), chip_rows)
                vals = x1_all[h * tiles + t, rs, :].astype(f32)
                sq = vals * vals
                tot = sq[:, 0:128]
                for k in range(1, tile // 128):
                    tot += sq[:, k * 128:(k + 1) * 128]
                ssq[rs, :] += tot
                xg[rs, h * tile:(h + 1) * tile] = (vals * gain_s[:, pl.ds(pl.multiple_of(h * half + t * tile, 128), tile)]).astype(bf16)
        for copy in wgu_copies(t):
            copy.wait()

        @pl.loop(0, 2 * ffn // 256)
        def _(i):
            cs = pl.ds(pl.multiple_of(i * 256, 256), 256)
            acc[:, cs] += jnp.dot(xg[...], wgu_buf[slot, :, cs], preferred_element_type=f32)

    last_hop = GATHER_LAG * reach_max

    def gather_round(j, carry):
        @pl.when(j < tiles)
        def _():
            produce(j)
        for h in range(1, reach_max + 1):
            t = j - GATHER_LAG * h

            @pl.when((t >= 0) & (t < tiles))
            def _():
                forward(t, h)
        t_use = j - last_hop - 1

        @pl.when((t_use >= 0) & (t_use < tiles))
        def _():
            consume(t_use)
        t_next = j - last_hop + 1

        @pl.when((t_next >= 0) & (t_next < tiles))
        def _():
            for copy in wgu_copies(t_next):
                copy.start()

        @pl.when((t_next >= 0) & (t_next < tiles))
        def _():
            wd_copy(t_next).start()
            wd_push(t_next).start()
        return carry

    lax.fori_loop(0, tiles + last_hop + 1, gather_round, 0)

    act_mine = pl.ds(pl.multiple_of(core * ffn, 128), ffn)
    act_theirs = pl.ds(pl.multiple_of(other * ffn, 128), ffn)

    def act_copy(b):
        ref = act_all.at[pl.ds(pl.multiple_of(b * chip_rows, chip_rows), chip_rows), act_mine]
        return remote(ref, ref, a_send.at[b], a_recv.at[b], partner)

    def act_arrival(b):
        ref = act_all.at[pl.ds(pl.multiple_of(b * chip_rows, chip_rows), chip_rows), act_theirs]
        return remote(ref, ref, a_send.at[b], a_recv.at[b], partner)

    @pl.loop(0, chips)
    def _(b):
        rs = pl.ds(pl.multiple_of(b * chip_rows, chip_rows), chip_rows)
        inv = lax.rsqrt(jnp.sum(ssq[rs, :], axis=1, keepdims=True) / width + EPS)
        gate = acc[rs, 0:ffn] * inv * gain_top
        upv = acc[rs, ffn:2 * ffn] * inv * gain_top
        act_all[rs, act_mine] = (gate / (1.0 + jnp.exp(-gate)) * upv).astype(bf16)
        act_copy(b).start()

    @pl.loop(0, chips)
    def _(b):
        act_arrival(b).wait_recv()

    ring_bufs = (ring_up, ring_dn)
    stage_bufs = (stage_up, stage_dn)

    def rows_of(c):
        return pl.ds(pl.multiple_of(c * chip_rows, chip_rows), chip_rows)

    def sum_copy(t, s, d):
        src = stage_bufs[d].at[t] if s == 1 else ring_bufs[d].at[t, s - 2]
        return remote(src, ring_bufs[d].at[t, s - 1], r_send.at[d, t, s - 1], r_recv.at[d, t, s - 1], upper if d == 0 else lower)

    def target(t, s, d):
        ahead = reach(t, d) - s + 1
        return lax.rem(chip + ahead, chips) if d == 0 else lax.rem(chip + chips - ahead, chips)

    def out_copy(t):
        return remote(stage_out.at[t], out_ref.at[:, pl.ds(pl.multiple_of(mine + t * tile, 128), tile)], f_send.at[t], f_recv.at[t], partner)

    def out_arrival(t):
        return remote(stage_out.at[t], out_ref.at[:, pl.ds(pl.multiple_of(theirs + t * tile, 128), tile)], f_send.at[t], f_recv.at[t], partner)

    def finish(t):
        slot = lax.rem(t, depth)
        for d in range(2):
            for s in range(1, reach_max + 1):
                @pl.when(s == reach(t, d))
                def _():
                    sum_copy(t, s, d).wait_recv()

        def total(c):
            near = pl.ds(pl.multiple_of(c * rows, rows), rows)
            far = pl.ds(pl.multiple_of(chip * chip_rows + c * rows, rows), rows)
            val = part[slot, far, :]
            for d in range(2):
                val += ring_bufs[d][t, reach(t, d) - 1, near, :].astype(f32)
            return (x1_all[core * tiles + t, far, :].astype(f32) + val).astype(bf16)

        stage_out[t] = total(other)
        out_copy(t).start()
        out_ref[:, pl.ds(pl.multiple_of(mine + t * tile, 128), tile)] = total(core)

    def scatter_round(j, carry):
        @pl.when(j < tiles)
        def _():
            slot = lax.rem(j, depth)
            wd_copy(j).wait()
            wd_arrival(j).wait_recv()

            @pl.loop(0, tile // 256)
            def _(i):
                cs = pl.ds(pl.multiple_of(i * 256, 256), 256)
                part[slot, :, cs] = jnp.dot(act_all[...], wd_all[j, :, cs], preferred_element_type=f32)
            for d in range(2):
                stage_bufs[d][j] = part[slot, rows_of(target(j, 1, d)), :].astype(bf16)
                sum_copy(j, 1, d).start()
        for s in range(2, reach_max + 1):
            t = j - SCATTER_LAG * (s - 1)

            @pl.when((t >= 0) & (t < tiles))
            def _():
                for d in range(2):
                    @pl.when(s <= reach(t, d))
                    def _():
                        sum_copy(t, s - 1, d).wait_recv()
                        buf = ring_bufs[d]
                        own = part[lax.rem(t, depth), rows_of(target(t, s, d)), :]
                        buf[t, s - 2] = (buf[t, s - 2].astype(f32) + own).astype(bf16)
                        sum_copy(t, s, d).start()
        t_end = j - SCATTER_LAG * reach_max

        @pl.when((t_end >= 0) & (t_end < tiles))
        def _():
            finish(t_end)
        return carry

    lax.fori_loop(0, tiles + SCATTER_LAG * reach_max, scatter_round, 0)

    o_push.wait_send()
    x_push.wait_send()

    @pl.loop(0, chips)
    def _(b):
        act_copy(b).wait_send()

    @pl.loop(0, tiles)
    def _(t):
        out_arrival(t).wait_recv()
        out_copy(t).wait_send()
        wd_push(t).wait_send()
        whole = x1_all.at[core * tiles + t]
        remote(whole, whole, p_send.at[t], p_recv.at[t], partner).wait_send()
        for d in range(2):
            for h in range(1, reach_max + 1):
                @pl.when(h <= reach(t, d))
                def _():
                    ring_copy(t, chip, h, d).wait_send()
                    sum_copy(t, h, d).wait_send()


def fused_tail(n, head_out, hidden, mlp_norm, w_out, w_gate, w_up, w_down, tile=256, sub=256):
    bf16, f32 = jnp.bfloat16, jnp.float32
    rows, width = hidden.shape
    inner = head_out.shape[1]
    ffn = w_gate.shape[1]
    half = width // 2
    tiles = half // tile
    chips = n // 2
    reach = chips // 2
    group = rows * n
    depth = min(tiles, SCATTER_LAG * reach + 1)
    dma = pltpu.SemaphoreType.DMA
    vmem = pl.BlockSpec(memory_space=pltpu.VMEM)
    hbm = pl.BlockSpec(memory_space=pl.ANY)
    scratch = [
        pltpu.VMEM((2 * rows, inner), bf16),
        pltpu.VMEM((2 * rows, half), bf16),
        pltpu.VMEM((1, width), f32),
        pltpu.VMEM((2, inner, sub), bf16),
        pltpu.VMEM((2, 2 * tile, 2 * ffn), bf16),
        pltpu.VMEM((2 * tiles, group, tile), bf16),
        pltpu.VMEM((group, 2 * tile), bf16),
        pltpu.VMEM((group, 2 * ffn), f32),
        pltpu.VMEM((group, 128), f32),
        pltpu.VMEM((group, 2 * ffn), bf16),
        pltpu.VMEM((tiles, 2 * ffn, tile), bf16),
        pltpu.VMEM((depth, group, tile), f32),
        pltpu.VMEM((tiles, 2 * rows, tile), bf16),
        pltpu.VMEM((tiles, 2 * rows, tile), bf16),
        pltpu.VMEM((tiles, reach, 2 * rows, tile), bf16),
        pltpu.VMEM((tiles, reach, 2 * rows, tile), bf16),
        pltpu.VMEM((tiles, rows, tile), bf16),
        dma((2,)), dma((2,)), dma((2,)), dma((2, 4)), dma((tiles,)), dma((tiles,)), dma((tiles,)),
        dma((2, tiles, reach)), dma((2, tiles, reach)), dma((tiles,)), dma((tiles,)),
        dma((chips,)), dma((chips,)), dma((2, tiles, reach)), dma((2, tiles, reach)), dma((tiles,)), dma((tiles,)),
    ]
    return pl.pallas_call(
        functools.partial(tail_kernel, n, tile, sub),
        out_shape=jax.ShapeDtypeStruct((rows, width), bf16),
        in_specs=[vmem, vmem, vmem, hbm, hbm, hbm, hbm],
        out_specs=vmem,
        scratch_shapes=scratch,
        compiler_params=pltpu.CompilerParams(collective_id=0, has_side_effects=True, vmem_limit_bytes=67_043_328),
        name='tail',
    )(head_out, hidden, mlp_norm.reshape(1, width), w_out, w_gate, w_up, w_down)


def solution(mesh):
    rows_spec = P(('dp', 'tp'), None)
    cache_spec = P(('dp', 'tp'), None, None)
    whole = P()
    in_specs = (rows_spec, cache_spec, cache_spec, P(('dp', 'tp')), whole, whole, whole, whole, whole, whole, whole, whole, P(None, 'tp'), P(None, 'tp'), P('tp', None))
    out_specs = (rows_spec, rows_spec, rows_spec)

    def device_step(hidden, cache_lat, cache_rope, seq_lens, attn_norm, w_query, w_kv_down, kv_norm, w_key_up, w_val_up, w_out, mlp_norm, w_gate, w_up, w_down):
        head_out, lat_new, rope_new = attention_block(hidden, cache_lat, cache_rope, seq_lens, attn_norm, w_query, w_kv_down, kv_norm, w_key_up, w_val_up)
        out_hidden = fused_tail(mesh.shape['tp'], head_out, hidden, mlp_norm, w_out, w_gate, w_up, w_down)
        return out_hidden, lat_new, rope_new

    return jax.shard_map(device_step, mesh=mesh, in_specs=in_specs, out_specs=out_specs, check_vma=False)
```

```python
import functools

import jax
import jax.numpy as jnp
from jax import lax
from jax.experimental import pallas as pl
from jax.experimental.pallas import tpu as pltpu
from jax.sharding import PartitionSpec as P

EPS = 1e-6
ROPE_BASE = 10000.0
value_a7 = 512
ROPE_DIM = 64
NOPE_DIM = 128
SCALE = (NOPE_DIM + ROPE_DIM) ** -0.5


def rms_norm(vals, gain):
    vals32 = vals.astype(jnp.float32)
    inv_rms = lax.rsqrt(jnp.mean(vals32 * vals32, axis=-1, keepdims=True) + EPS)
    return (vals32 * inv_rms * gain.astype(jnp.float32)).astype(jnp.bfloat16)


def rotate(vals, cos_tab, sin_tab):
    half = vals.shape[-1] // 2
    first = vals[..., :half]
    second = vals[..., half:]
    return jnp.concatenate([first * cos_tab - second * sin_tab, second * cos_tab + first * sin_tab], axis=-1)


def rope_tables(seq_lens):
    inv_freq = ROPE_BASE ** (-jnp.arange(0, ROPE_DIM, 2, dtype=jnp.float32) / ROPE_DIM)
    angles = seq_lens.astype(jnp.float32)[:, None] * inv_freq[None, :]
    return jnp.cos(angles), jnp.sin(angles)


def attention_block(hidden, cache_lat, cache_rope, seq_lens, attn_norm, w_query, w_kv_down, kv_norm, w_key_up, w_val_up):
    rows = hidden.shape[0]
    heads = w_key_up.shape[1] // NOPE_DIM
    query, kv_proj = paired_query(hidden, attn_norm, w_query, w_kv_down)
    query = query.reshape(rows, heads, NOPE_DIM + ROPE_DIM)
    lat_new = rms_norm(kv_proj[:, :value_a7], kv_norm)
    cos_tab, sin_tab = rope_tables(seq_lens)
    rope_new = rotate(kv_proj[:, value_a7:].astype(jnp.float32), cos_tab, sin_tab).astype(jnp.bfloat16)
    q_rot = rotate(query[:, :, NOPE_DIM:].astype(jnp.float32), cos_tab[:, None, :], sin_tab[:, None, :]).astype(jnp.bfloat16)
    key_up = w_key_up.reshape(value_a7, heads, NOPE_DIM)
    q_lat = jnp.einsum('bhn,khn->bhk', query[:, :, :NOPE_DIM], key_up, preferred_element_type=jnp.float32).astype(jnp.bfloat16)
    scores = (jnp.einsum('bhk,bsk->bhs', q_lat, cache_lat, preferred_element_type=jnp.float32) + jnp.einsum('bhr,bsr->bhs', q_rot, cache_rope, preferred_element_type=jnp.float32)) * SCALE
    score_new = (jnp.einsum('bhk,bk->bh', q_lat, lat_new, preferred_element_type=jnp.float32) + jnp.einsum('bhr,br->bh', q_rot, rope_new, preferred_element_type=jnp.float32)) * SCALE
    slots = cache_lat.shape[1]
    valid = jnp.arange(slots)[None, None, :] < seq_lens[:, None, None]
    scores = jnp.where(valid, scores, -jnp.inf)
    top = jnp.maximum(jnp.max(scores, axis=-1), score_new)
    expo = jnp.exp(scores - top[..., None])
    expo_new = jnp.exp(score_new - top)
    denom = jnp.sum(expo, axis=-1) + expo_new
    probs = (expo / denom[..., None]).astype(jnp.bfloat16)
    prob_new = (expo_new / denom).astype(jnp.bfloat16)
    lat_sum = jnp.einsum('bhs,bsk->bhk', probs, cache_lat, preferred_element_type=jnp.float32) + prob_new.astype(jnp.float32)[..., None] * lat_new.astype(jnp.float32)[:, None, :]
    lat_out = lat_sum.astype(jnp.bfloat16)
    head_out = head_values(jnp.swapaxes(lat_out, 0, 1), w_val_up)
    return head_out, lat_new, rope_new

MESH = pl.DeviceIdType.MESH
GATHER_LAG = 1
SCATTER_LAG = 2

def head_kernel(lat_ref, val_ref, out_ref):
    heads = lat_ref.shape[0]
    dim = val_ref.shape[1] // heads
    for h in range(heads):
        cols = slice(h * dim, (h + 1) * dim)
        out_ref[:, cols] = jnp.dot(lat_ref[h], val_ref[:, cols], preferred_element_type=jnp.float32).astype(jnp.bfloat16)


def head_values(lat_out, w_val_up, step=8):
    heads, rows, depth = lat_out.shape
    cols = w_val_up.shape[1] // heads * step
    return pl.pallas_call(
        head_kernel,
        out_shape=jax.ShapeDtypeStruct((rows, w_val_up.shape[1]), jnp.bfloat16),
        grid=(heads // step,),
        in_specs=[pl.BlockSpec((step, rows, depth), lambda i: (i, 0, 0)), pl.BlockSpec((depth, cols), lambda i: (0, i))],
        out_specs=pl.BlockSpec((rows, cols), lambda i: (0, i)),
        cost_estimate=pl.CostEstimate(flops=2 * rows * depth * w_val_up.shape[1], bytes_accessed=2 * depth * w_val_up.shape[1], transcendentals=0),
        name='head_values',
    )(lat_out, w_val_up)


def query_kernel(sub, x_ref, gain_ref, wq_hbm, wkv_hbm, q_ref, kv_ref,
                 h_all, w_buf, wkv_buf, stage, kv_part, kv_stage, kv_in,
                 w_sem, wkv_sem, h_send, h_recv, k_send, k_recv, q_send, q_recv):
    f32, bf16 = jnp.float32, jnp.bfloat16
    rows, width = x_ref.shape
    half = width // 2
    q_half = wq_hbm.shape[1] // 2
    tiles = q_half // sub
    slots = w_buf.shape[0]
    me = lax.axis_index('tp')
    core = lax.rem(me, 2)
    other = 1 - core
    partner = me + 1 - 2 * core
    my_rows = pl.ds(pl.multiple_of(core * rows, rows), rows)
    their_rows = pl.ds(pl.multiple_of(other * rows, rows), rows)
    my_depth = pl.ds(pl.multiple_of(core * half, 128), half)

    def remote(src, dst, send_sem, recv_sem):
        return pltpu.make_async_remote_copy(src_ref=src, dst_ref=dst, send_sem=send_sem, recv_sem=recv_sem, device_id={'tp': partner}, device_id_type=MESH)

    def w_copy(i):
        slot = lax.rem(i, slots)
        return pltpu.make_async_copy(wq_hbm.at[:, pl.ds(pl.multiple_of(core * q_half + i * sub, 128), sub)], w_buf.at[slot], w_sem.at[slot])

    wkv_copy = pltpu.make_async_copy(wkv_hbm.at[:, my_depth], wkv_buf, wkv_sem.at[0])
    wkv_copy.start()
    for i in range(slots):
        w_copy(i).start()

    barrier = pltpu.get_barrier_semaphore()
    pl.semaphore_signal(barrier, inc=1, device_id={'tp': partner}, device_id_type=MESH)

    step = min(1024, width)
    tot = jnp.zeros((rows, 128), f32)
    for c in range(0, width, step):
        vals = x_ref[:, c:c + step].astype(f32)
        sq = vals * vals
        for k in range(0, step, 128):
            tot += sq[:, k:k + 128]
    inv = lax.rsqrt(jnp.sum(tot, axis=1, keepdims=True) / width + EPS)
    for c in range(0, width, step):
        vals = x_ref[:, c:c + step].astype(f32)
        h_all[my_rows, c:c + step] = (vals * inv * gain_ref[:, c:c + step].astype(f32)).astype(bf16)

    pl.semaphore_wait(barrier, 1)
    h_push = remote(h_all.at[my_rows, :], h_all.at[my_rows, :], h_send.at[0], h_recv.at[0])
    h_push.start()
    remote(h_all.at[their_rows, :], h_all.at[their_rows, :], h_send.at[0], h_recv.at[0]).wait_recv()

    wkv_copy.wait()
    kv_part[...] = lax.dot_general(h_all[:, my_depth], wkv_buf[...], (((1,), (1,)), ((), ())), preferred_element_type=f32)
    kv_stage[...] = kv_part[their_rows, :]
    kv_push = remote(kv_stage, kv_in, k_send.at[0], k_recv.at[0])
    kv_push.start()

    def cols_of(c, i):
        return pl.ds(pl.multiple_of(c * q_half + i * sub, 128), sub)

    def q_copy(i):
        return remote(stage.at[i], q_ref.at[:, cols_of(core, i)], q_send.at[i], q_recv.at[i])

    @pl.loop(0, tiles)
    def _(i):
        slot = lax.rem(i, slots)
        w_copy(i).wait()
        prod = jnp.dot(h_all[...], w_buf[slot], preferred_element_type=f32).astype(bf16)

        @pl.when(i + slots < tiles)
        def _():
            w_copy(i + slots).start()
        low, high = prod[0:rows], prod[rows:2 * rows]
        first = core == 0
        q_ref[:, cols_of(core, i)] = jnp.where(first, low, high)
        stage[i] = jnp.where(first, high, low)
        q_copy(i).start()

    kv_push.wait_recv()
    kv_ref[...] = (kv_part[my_rows, :] + kv_in[...]).astype(bf16)
    h_push.wait_send()
    kv_push.wait_send()

    @pl.loop(0, tiles)
    def _(i):
        q_copy(i).wait_send()
        remote(stage.at[i], q_ref.at[:, cols_of(other, i)], q_send.at[i], q_recv.at[i]).wait_recv()


def paired_query(hidden, attn_norm, w_query, w_kv_down, sub=256):
    bf16, f32 = jnp.bfloat16, jnp.float32
    rows, width = hidden.shape
    q_cols = w_query.shape[1]
    kv_cols = w_kv_down.shape[1]
    tiles = q_cols // 2 // sub
    slots = min(8, tiles)
    dma = pltpu.SemaphoreType.DMA
    vmem = pl.BlockSpec(memory_space=pltpu.VMEM)
    hbm = pl.BlockSpec(memory_space=pl.ANY)
    scratch = [
        pltpu.VMEM((2 * rows, width), bf16),
        pltpu.VMEM((slots, width, sub), bf16),
        pltpu.VMEM((kv_cols, width // 2), bf16),
        pltpu.VMEM((tiles, rows, sub), bf16),
        pltpu.VMEM((2 * rows, kv_cols), f32),
        pltpu.VMEM((rows, kv_cols), f32),
        pltpu.VMEM((rows, kv_cols), f32),
        dma((slots,)), dma((1,)), dma((1,)), dma((1,)), dma((1,)), dma((1,)), dma((tiles,)), dma((tiles,)),
    ]
    return pl.pallas_call(
        functools.partial(query_kernel, sub),
        out_shape=(jax.ShapeDtypeStruct((rows, q_cols), bf16), jax.ShapeDtypeStruct((rows, kv_cols), bf16)),
        in_specs=[vmem, vmem, hbm, hbm],
        out_specs=(vmem, vmem),
        scratch_shapes=scratch,
        compiler_params=pltpu.CompilerParams(collective_id=1, has_side_effects=True, vmem_limit_bytes=60_000_000),
        name='query',
    )(hidden, attn_norm.reshape(1, width), w_query, w_kv_down.T)


def tail_kernel(n, tile, sub, o_ref, x_ref, gain_ref, wo_hbm, wg_hbm, wu_hbm, wd_hbm, out_ref,
                o_all, x_half, gain_s, wo_buf, wgu_buf, x1_all, xg, acc, ssq, act_all, wd_all, part,
                stage_up, stage_dn, ring_up, ring_dn, stage_out,
                pre_send, pre_recv, wo_sem, wgu_sem, wd_sem, wdp_send, wdp_recv,
                g_send, g_recv, p_send, p_recv, a_send, a_recv, r_send, r_recv, f_send, f_recv):
    f32, bf16 = jnp.float32, jnp.bfloat16
    rows, width = x_ref.shape
    half = width // 2
    tiles = half // tile
    subs = tile // sub
    ffn = wg_hbm.shape[1]
    chips = n // 2
    reach_max = chips // 2
    chip_rows = 2 * rows
    depth = part.shape[0]

    me = lax.axis_index('tp')
    core = lax.rem(me, 2)
    chip = lax.div(me, 2)
    other = 1 - core
    partner = me + 1 - 2 * core
    upper = lax.rem(me + 2, n)
    lower = lax.rem(me + n - 2, n)
    mine = pl.multiple_of(core * half, 128)
    theirs = pl.multiple_of(other * half, 128)

    def remote(src, dst, send_sem, recv_sem, dev):
        return pltpu.make_async_remote_copy(src_ref=src, dst_ref=dst, send_sem=send_sem, recv_sem=recv_sem, device_id={'tp': dev}, device_id_type=MESH)

    def wo_copy(i):
        slot = lax.rem(i, 2)
        return pltpu.make_async_copy(wo_hbm.at[:, pl.ds(pl.multiple_of(mine + i * sub, 128), sub)], wo_buf.at[slot], wo_sem.at[slot])

    def wgu_copies(t):
        slot = lax.rem(t, 2)
        out = []
        for h in range(2):
            for k, src in enumerate((wg_hbm, wu_hbm)):
                out.append(pltpu.make_async_copy(src.at[pl.ds(pl.multiple_of(h * half + t * tile, 128), tile), :], wgu_buf.at[slot, pl.ds(h * tile, tile), pl.ds(k * ffn, ffn)], wgu_sem.at[slot, 2 * h + k]))
        return out

    def wd_copy(t):
        return pltpu.make_async_copy(wd_hbm.at[:, pl.ds(pl.multiple_of(mine + t * tile, 128), tile)], wd_all.at[t, pl.ds(pl.multiple_of(core * ffn, 128), ffn), :], wd_sem.at[t])

    def wd_push(t):
        return remote(wd_hbm.at[:, pl.ds(pl.multiple_of(theirs + t * tile, 128), tile)], wd_all.at[t, pl.ds(pl.multiple_of(core * ffn, 128), ffn), :], wdp_send.at[t], wdp_recv.at[t], partner)

    def wd_arrival(t):
        return remote(wd_hbm.at[:, pl.ds(0, tile)], wd_all.at[t, pl.ds(pl.multiple_of(other * ffn, 128), ffn), :], wdp_send.at[t], wdp_recv.at[t], partner)

    wo_copy(0).start()
    wo_copy(1).start()

    barrier = pltpu.get_barrier_semaphore()
    for dev in (partner, upper, lower):
        pl.semaphore_signal(barrier, inc=1, device_id={'tp': dev}, device_id_type=MESH)
    pl.semaphore_wait(barrier, 3)

    my_rows = pl.ds(pl.multiple_of(core * rows, rows), rows)
    their_rows = pl.ds(pl.multiple_of(other * rows, rows), rows)
    o_push = remote(o_ref, o_all.at[my_rows, :], pre_send.at[0], pre_recv.at[0], partner)
    x_push = remote(x_ref.at[:, pl.ds(theirs, half)], x_half.at[my_rows, :], pre_send.at[1], pre_recv.at[1], partner)
    o_push.start()
    x_push.start()
    o_all[my_rows, :] = o_ref[...]
    x_half[my_rows, :] = x_ref[:, pl.ds(mine, half)]
    gain = gain_ref[...].astype(f32)
    gain_top = jnp.maximum(jnp.max(jnp.abs(gain), axis=1, keepdims=True), 1e-30)
    gain_s[...] = gain / gain_top
    acc[...] = jnp.zeros_like(acc)
    ssq[...] = jnp.zeros_like(ssq)
    remote(o_ref, o_all.at[their_rows, :], pre_send.at[0], pre_recv.at[0], partner).wait_recv()
    remote(x_ref.at[:, pl.ds(theirs, half)], x_half.at[their_rows, :], pre_send.at[1], pre_recv.at[1], partner).wait_recv()

    def reach(t, d):
        first = reach_max - lax.rem(t, 2)
        return first if d == 0 else chips - 1 - first

    def origin(h, d):
        return lax.rem(chip + chips - h, chips) if d == 0 else lax.rem(chip + h, chips)

    def block(t, src):
        return x1_all.at[core * tiles + t, pl.ds(pl.multiple_of(src * chip_rows, chip_rows), chip_rows), :]

    def ring_copy(t, src, hop, d):
        return remote(block(t, src), block(t, src), g_send.at[d, t, hop - 1], g_recv.at[d, t, hop - 1], upper if d == 0 else lower)

    def pair_copy(t, src):
        return remote(block(t, src), block(t, src), p_send.at[t], p_recv.at[t], partner)

    def produce(t):
        for q in range(subs):
            i = t * subs + q
            slot = lax.rem(i, 2)
            wo_copy(i).wait()
            prod = jnp.dot(o_all[...], wo_buf[slot], preferred_element_type=f32)
            x1 = (x_half[:, pl.ds(pl.multiple_of(i * sub, 128), sub)].astype(f32) + prod).astype(bf16)
            x1_all[core * tiles + t, pl.ds(pl.multiple_of(chip * chip_rows, chip_rows), chip_rows), pl.ds(q * sub, sub)] = x1

            @pl.when(i + 2 < tiles * subs)
            def _():
                wo_copy(i + 2).start()
        for d in range(2):
            ring_copy(t, chip, 1, d).start()
        pair_copy(t, chip).start()

    def forward(t, h):
        for d in range(2):
            @pl.when(h <= reach(t, d))
            def _():
                src = origin(h, d)
                ring_copy(t, src, h, d).wait_recv()

                @pl.when(h < reach(t, d))
                def _():
                    ring_copy(t, src, h + 1, d).start()
                pair_copy(t, src).start()

    def consume(t):
        slot = lax.rem(t, 2)
        whole = x1_all.at[other * tiles + t]
        remote(whole, whole, p_send.at[t], p_recv.at[t], partner).wait_recv()
        for h in range(2):
            @pl.loop(0, chips)
            def _(b):
                rs = pl.ds(pl.multiple_of(b * chip_rows, chip_rows), chip_rows)
                vals = x1_all[h * tiles + t, rs, :].astype(f32)
                sq = vals * vals
                tot = sq[:, 0:128]
                for k in range(1, tile // 128):
                    tot += sq[:, k * 128:(k + 1) * 128]
                ssq[rs, :] += tot
                xg[rs, h * tile:(h + 1) * tile] = (vals * gain_s[:, pl.ds(pl.multiple_of(h * half + t * tile, 128), tile)]).astype(bf16)
        for copy in wgu_copies(t):
            copy.wait()

        @pl.loop(0, 2 * ffn // 256)
        def _(i):
            cs = pl.ds(pl.multiple_of(i * 256, 256), 256)
            acc[:, cs] += jnp.dot(xg[...], wgu_buf[slot, :, cs], preferred_element_type=f32)

    last_hop = GATHER_LAG * reach_max

    def gather_round(j, carry):
        @pl.when(j < tiles)
        def _():
            produce(j)
        for h in range(1, reach_max + 1):
            t = j - GATHER_LAG * h

            @pl.when((t >= 0) & (t < tiles))
            def _():
                forward(t, h)
        t_use = j - last_hop - 1

        @pl.when((t_use >= 0) & (t_use < tiles))
        def _():
            consume(t_use)
        t_next = j - last_hop + 1

        @pl.when((t_next >= 0) & (t_next < tiles))
        def _():
            for copy in wgu_copies(t_next):
                copy.start()

        @pl.when((t_next >= 0) & (t_next < tiles))
        def _():
            wd_copy(t_next).start()
            wd_push(t_next).start()
        return carry

    lax.fori_loop(0, tiles + last_hop + 1, gather_round, 0)

    act_mine = pl.ds(pl.multiple_of(core * ffn, 128), ffn)
    act_theirs = pl.ds(pl.multiple_of(other * ffn, 128), ffn)

    def act_copy(b):
        ref = act_all.at[pl.ds(pl.multiple_of(b * chip_rows, chip_rows), chip_rows), act_mine]
        return remote(ref, ref, a_send.at[b], a_recv.at[b], partner)

    def act_arrival(b):
        ref = act_all.at[pl.ds(pl.multiple_of(b * chip_rows, chip_rows), chip_rows), act_theirs]
        return remote(ref, ref, a_send.at[b], a_recv.at[b], partner)

    @pl.loop(0, chips)
    def _(b):
        rs = pl.ds(pl.multiple_of(b * chip_rows, chip_rows), chip_rows)
        inv = lax.rsqrt(jnp.sum(ssq[rs, :], axis=1, keepdims=True) / width + EPS)
        gate = acc[rs, 0:ffn] * inv * gain_top
        upv = acc[rs, ffn:2 * ffn] * inv * gain_top
        act_all[rs, act_mine] = (gate / (1.0 + jnp.exp(-gate)) * upv).astype(bf16)
        act_copy(b).start()

    @pl.loop(0, chips)
    def _(b):
        act_arrival(b).wait_recv()

    ring_bufs = (ring_up, ring_dn)
    stage_bufs = (stage_up, stage_dn)

    def rows_of(c):
        return pl.ds(pl.multiple_of(c * chip_rows, chip_rows), chip_rows)

    def sum_copy(t, s, d):
        src = stage_bufs[d].at[t] if s == 1 else ring_bufs[d].at[t, s - 2]
        return remote(src, ring_bufs[d].at[t, s - 1], r_send.at[d, t, s - 1], r_recv.at[d, t, s - 1], upper if d == 0 else lower)

    def target(t, s, d):
        ahead = reach(t, d) - s + 1
        return lax.rem(chip + ahead, chips) if d == 0 else lax.rem(chip + chips - ahead, chips)

    def out_copy(t):
        return remote(stage_out.at[t], out_ref.at[:, pl.ds(pl.multiple_of(mine + t * tile, 128), tile)], f_send.at[t], f_recv.at[t], partner)

    def out_arrival(t):
        return remote(stage_out.at[t], out_ref.at[:, pl.ds(pl.multiple_of(theirs + t * tile, 128), tile)], f_send.at[t], f_recv.at[t], partner)

    def finish(t):
        slot = lax.rem(t, depth)
        for d in range(2):
            for s in range(1, reach_max + 1):
                @pl.when(s == reach(t, d))
                def _():
                    sum_copy(t, s, d).wait_recv()

        def total(c):
            near = pl.ds(pl.multiple_of(c * rows, rows), rows)
            far = pl.ds(pl.multiple_of(chip * chip_rows + c * rows, rows), rows)
            val = part[slot, far, :]
            for d in range(2):
                val += ring_bufs[d][t, reach(t, d) - 1, near, :].astype(f32)
            return (x1_all[core * tiles + t, far, :].astype(f32) + val).astype(bf16)

        stage_out[t] = total(other)
        out_copy(t).start()
        out_ref[:, pl.ds(pl.multiple_of(mine + t * tile, 128), tile)] = total(core)

    def scatter_round(j, carry):
        @pl.when(j < tiles)
        def _():
            slot = lax.rem(j, depth)
            wd_copy(j).wait()
            wd_arrival(j).wait_recv()

            @pl.loop(0, tile // 256)
            def _(i):
                cs = pl.ds(pl.multiple_of(i * 256, 256), 256)
                part[slot, :, cs] = jnp.dot(act_all[...], wd_all[j, :, cs], preferred_element_type=f32)
            for d in range(2):
                stage_bufs[d][j] = part[slot, rows_of(target(j, 1, d)), :].astype(bf16)
                sum_copy(j, 1, d).start()
        for s in range(2, reach_max + 1):
            t = j - SCATTER_LAG * (s - 1)

            @pl.when((t >= 0) & (t < tiles))
            def _():
                for d in range(2):
                    @pl.when(s <= reach(t, d))
                    def _():
                        sum_copy(t, s - 1, d).wait_recv()
                        buf = ring_bufs[d]
                        own = part[lax.rem(t, depth), rows_of(target(t, s, d)), :]
                        buf[t, s - 2] = (buf[t, s - 2].astype(f32) + own).astype(bf16)
                        sum_copy(t, s, d).start()
        t_end = j - SCATTER_LAG * reach_max

        @pl.when((t_end >= 0) & (t_end < tiles))
        def _():
            finish(t_end)
        return carry

    lax.fori_loop(0, tiles + SCATTER_LAG * reach_max, scatter_round, 0)

    o_push.wait_send()
    x_push.wait_send()

    @pl.loop(0, chips)
    def _(b):
        act_copy(b).wait_send()

    @pl.loop(0, tiles)
    def _(t):
        out_arrival(t).wait_recv()
        out_copy(t).wait_send()
        wd_push(t).wait_send()
        whole = x1_all.at[core * tiles + t]
        remote(whole, whole, p_send.at[t], p_recv.at[t], partner).wait_send()
        for d in range(2):
            for h in range(1, reach_max + 1):
                @pl.when(h <= reach(t, d))
                def _():
                    ring_copy(t, chip, h, d).wait_send()
                    sum_copy(t, h, d).wait_send()


def fused_tail(n, head_out, hidden, mlp_norm, w_out, w_gate, w_up, w_down, tile=512, sub=256):
    bf16, f32 = jnp.bfloat16, jnp.float32
    rows, width = hidden.shape
    inner = head_out.shape[1]
    ffn = w_gate.shape[1]
    half = width // 2
    tiles = half // tile
    chips = n // 2
    reach = chips // 2
    group = rows * n
    depth = min(tiles, SCATTER_LAG * reach + 1)
    dma = pltpu.SemaphoreType.DMA
    vmem = pl.BlockSpec(memory_space=pltpu.VMEM)
    hbm = pl.BlockSpec(memory_space=pl.ANY)
    scratch = [
        pltpu.VMEM((2 * rows, inner), bf16),
        pltpu.VMEM((2 * rows, half), bf16),
        pltpu.VMEM((1, width), f32),
        pltpu.VMEM((2, inner, sub), bf16),
        pltpu.VMEM((2, 2 * tile, 2 * ffn), bf16),
        pltpu.VMEM((2 * tiles, group, tile), bf16),
        pltpu.VMEM((group, 2 * tile), bf16),
        pltpu.VMEM((group, 2 * ffn), f32),
        pltpu.VMEM((group, 128), f32),
        pltpu.VMEM((group, 2 * ffn), bf16),
        pltpu.VMEM((tiles, 2 * ffn, tile), bf16),
        pltpu.VMEM((depth, group, tile), f32),
        pltpu.VMEM((tiles, 2 * rows, tile), bf16),
        pltpu.VMEM((tiles, 2 * rows, tile), bf16),
        pltpu.VMEM((tiles, reach, 2 * rows, tile), bf16),
        pltpu.VMEM((tiles, reach, 2 * rows, tile), bf16),
        pltpu.VMEM((tiles, rows, tile), bf16),
        dma((2,)), dma((2,)), dma((2,)), dma((2, 4)), dma((tiles,)), dma((tiles,)), dma((tiles,)),
        dma((2, tiles, reach)), dma((2, tiles, reach)), dma((tiles,)), dma((tiles,)),
        dma((chips,)), dma((chips,)), dma((2, tiles, reach)), dma((2, tiles, reach)), dma((tiles,)), dma((tiles,)),
    ]
    return pl.pallas_call(
        functools.partial(tail_kernel, n, tile, sub),
        out_shape=jax.ShapeDtypeStruct((rows, width), bf16),
        in_specs=[vmem, vmem, vmem, hbm, hbm, hbm, hbm],
        out_specs=vmem,
        scratch_shapes=scratch,
        compiler_params=pltpu.CompilerParams(collective_id=0, has_side_effects=True, vmem_limit_bytes=67_043_328),
        name='tail',
    )(head_out, hidden, mlp_norm.reshape(1, width), w_out, w_gate, w_up, w_down)


def solution(mesh):
    rows_spec = P(('dp', 'tp'), None)
    cache_spec = P(('dp', 'tp'), None, None)
    whole = P()
    in_specs = (rows_spec, cache_spec, cache_spec, P(('dp', 'tp')), whole, whole, whole, whole, whole, whole, whole, whole, P(None, 'tp'), P(None, 'tp'), P('tp', None))
    out_specs = (rows_spec, rows_spec, rows_spec)

    def device_step(hidden, cache_lat, cache_rope, seq_lens, attn_norm, w_query, w_kv_down, kv_norm, w_key_up, w_val_up, w_out, mlp_norm, w_gate, w_up, w_down):
        head_out, lat_new, rope_new = attention_block(hidden, cache_lat, cache_rope, seq_lens, attn_norm, w_query, w_kv_down, kv_norm, w_key_up, w_val_up)
        out_hidden = fused_tail(mesh.shape['tp'], head_out, hidden, mlp_norm, w_out, w_gate, w_up, w_down)
        return out_hidden, lat_new, rope_new

    return jax.shard_map(device_step, mesh=mesh, in_specs=in_specs, out_specs=out_specs, check_vma=False)
```

```python
import functools

import jax
import jax.numpy as jnp
from jax import lax
from jax.experimental import pallas as pl
from jax.experimental.pallas import tpu as pltpu
from jax.sharding import PartitionSpec as P

EPS = 1e-6
ROPE_BASE = 10000.0
value_a7 = 512
ROPE_DIM = 64
NOPE_DIM = 128
SCALE = (NOPE_DIM + ROPE_DIM) ** -0.5


def rms_norm(vals, gain):
    vals32 = vals.astype(jnp.float32)
    inv_rms = lax.rsqrt(jnp.mean(vals32 * vals32, axis=-1, keepdims=True) + EPS)
    return (vals32 * inv_rms * gain.astype(jnp.float32)).astype(jnp.bfloat16)


def rotate(vals, cos_tab, sin_tab):
    half = vals.shape[-1] // 2
    first = vals[..., :half]
    second = vals[..., half:]
    return jnp.concatenate([first * cos_tab - second * sin_tab, second * cos_tab + first * sin_tab], axis=-1)


def rope_tables(seq_lens):
    inv_freq = ROPE_BASE ** (-jnp.arange(0, ROPE_DIM, 2, dtype=jnp.float32) / ROPE_DIM)
    angles = seq_lens.astype(jnp.float32)[:, None] * inv_freq[None, :]
    return jnp.cos(angles), jnp.sin(angles)


def attention_block(hidden, cache_lat, cache_rope, seq_lens, attn_norm, w_query, w_kv_down, kv_norm, w_key_up, w_val_up):
    rows = hidden.shape[0]
    heads = w_key_up.shape[1] // NOPE_DIM
    query, kv_proj = paired_query(hidden, attn_norm, w_query, w_kv_down)
    query = query.reshape(rows, heads, NOPE_DIM + ROPE_DIM)
    lat_new = rms_norm(kv_proj[:, :value_a7], kv_norm)
    cos_tab, sin_tab = rope_tables(seq_lens)
    rope_new = rotate(kv_proj[:, value_a7:].astype(jnp.float32), cos_tab, sin_tab).astype(jnp.bfloat16)
    q_rot = rotate(query[:, :, NOPE_DIM:].astype(jnp.float32), cos_tab[:, None, :], sin_tab[:, None, :]).astype(jnp.bfloat16)
    key_up = w_key_up.reshape(value_a7, heads, NOPE_DIM)
    q_lat = jnp.einsum('bhn,khn->bhk', query[:, :, :NOPE_DIM], key_up, preferred_element_type=jnp.float32).astype(jnp.bfloat16)
    scores = (jnp.einsum('bhk,bsk->bhs', q_lat, cache_lat, preferred_element_type=jnp.float32) + jnp.einsum('bhr,bsr->bhs', q_rot, cache_rope, preferred_element_type=jnp.float32)) * SCALE
    score_new = (jnp.einsum('bhk,bk->bh', q_lat, lat_new, preferred_element_type=jnp.float32) + jnp.einsum('bhr,br->bh', q_rot, rope_new, preferred_element_type=jnp.float32)) * SCALE
    slots = cache_lat.shape[1]
    valid = jnp.arange(slots)[None, None, :] < seq_lens[:, None, None]
    scores = jnp.where(valid, scores, -jnp.inf)
    top = jnp.maximum(jnp.max(scores, axis=-1), score_new)
    expo = jnp.exp(scores - top[..., None])
    expo_new = jnp.exp(score_new - top)
    denom = jnp.sum(expo, axis=-1) + expo_new
    probs = (expo / denom[..., None]).astype(jnp.bfloat16)
    prob_new = (expo_new / denom).astype(jnp.bfloat16)
    lat_sum = jnp.einsum('bhs,bsk->bhk', probs, cache_lat, preferred_element_type=jnp.float32) + prob_new.astype(jnp.float32)[..., None] * lat_new.astype(jnp.float32)[:, None, :]
    head_out = head_values(lat_sum, w_val_up)
    return head_out, lat_new, rope_new

MESH = pl.DeviceIdType.MESH
GATHER_LAG = 1
SCATTER_LAG = 2

def head_kernel(heads, lat_ref, val_ref, out_ref, lat_buf):
    rows = out_ref.shape[0]
    width = val_ref.shape[1]
    dim = width // heads
    lanes, total, _ = lat_buf.shape
    quad, group = 4, 16
    step = total // 16

    @pl.loop(0, 16)
    def _(b):
        rs = pl.ds(pl.multiple_of(b * step, step), step)
        for i in range(lanes):
            lat_buf[i, rs, :] = lat_ref[rs, i * 128:(i + 1) * 128]

    @pl.loop(0, heads // group)
    def _(c):
        for g in range(group // quad):
            first = c * group + g * quad
            parts = [jnp.concatenate([lat_buf[i, pl.ds(first + k, rows, stride=heads), :] for k in range(quad)], axis=0) for i in range(lanes)]
            lhs = jnp.concatenate(parts, axis=1).astype(jnp.bfloat16)
            cols = pl.ds(pl.multiple_of(first * dim, quad * dim), quad * dim)
            prod = jnp.dot(lhs, val_ref[:, cols], preferred_element_type=jnp.float32)
            diag = [prod[k * rows:(k + 1) * rows, k * dim:(k + 1) * dim] for k in range(quad)]
            out_ref[:, cols] = jnp.concatenate(diag, axis=1).astype(jnp.bfloat16)


def head_values(lat_sum, w_val_up):
    rows, heads, depth = lat_sum.shape
    width = w_val_up.shape[1]
    vmem = pl.BlockSpec(memory_space=pltpu.VMEM)
    return pl.pallas_call(
        functools.partial(head_kernel, heads),
        out_shape=jax.ShapeDtypeStruct((rows, width), jnp.bfloat16),
        in_specs=[vmem, vmem],
        out_specs=vmem,
        scratch_shapes=[pltpu.VMEM((depth // 128, rows * heads, 128), jnp.float32)],
        cost_estimate=pl.CostEstimate(flops=2 * rows * depth * width, bytes_accessed=2 * depth * width, transcendentals=0),
        compiler_params=pltpu.CompilerParams(vmem_limit_bytes=24_000_000),
        name='head_values',
    )(lat_sum.reshape(rows * heads, depth), w_val_up)


def query_kernel(sub, x_ref, gain_ref, wq_hbm, wkv_hbm, q_ref, kv_ref,
                 h_all, w_buf, wkv_buf, stage, kv_part, kv_stage, kv_in,
                 w_sem, wkv_sem, h_send, h_recv, k_send, k_recv, q_send, q_recv):
    f32, bf16 = jnp.float32, jnp.bfloat16
    rows, width = x_ref.shape
    half = width // 2
    q_half = wq_hbm.shape[1] // 2
    tiles = q_half // sub
    slots = w_buf.shape[0]
    me = lax.axis_index('tp')
    core = lax.rem(me, 2)
    other = 1 - core
    partner = me + 1 - 2 * core
    my_rows = pl.ds(pl.multiple_of(core * rows, rows), rows)
    their_rows = pl.ds(pl.multiple_of(other * rows, rows), rows)
    my_depth = pl.ds(pl.multiple_of(core * half, 128), half)

    def remote(src, dst, send_sem, recv_sem):
        return pltpu.make_async_remote_copy(src_ref=src, dst_ref=dst, send_sem=send_sem, recv_sem=recv_sem, device_id={'tp': partner}, device_id_type=MESH)

    def w_copy(i):
        slot = lax.rem(i, slots)
        return pltpu.make_async_copy(wq_hbm.at[:, pl.ds(pl.multiple_of(core * q_half + i * sub, 128), sub)], w_buf.at[slot], w_sem.at[slot])

    wkv_copy = pltpu.make_async_copy(wkv_hbm.at[:, my_depth], wkv_buf, wkv_sem.at[0])
    wkv_copy.start()
    for i in range(slots):
        w_copy(i).start()

    barrier = pltpu.get_barrier_semaphore()
    pl.semaphore_signal(barrier, inc=1, device_id={'tp': partner}, device_id_type=MESH)

    step = min(1024, width)
    tot = jnp.zeros((rows, 128), f32)
    for c in range(0, width, step):
        vals = x_ref[:, c:c + step].astype(f32)
        sq = vals * vals
        for k in range(0, step, 128):
            tot += sq[:, k:k + 128]
    inv = lax.rsqrt(jnp.sum(tot, axis=1, keepdims=True) / width + EPS)
    for c in range(0, width, step):
        vals = x_ref[:, c:c + step].astype(f32)
        h_all[my_rows, c:c + step] = (vals * inv * gain_ref[c:c + step].astype(f32)[None, :]).astype(bf16)

    pl.semaphore_wait(barrier, 1)
    h_push = remote(h_all.at[my_rows, :], h_all.at[my_rows, :], h_send.at[0], h_recv.at[0])
    h_push.start()
    remote(h_all.at[their_rows, :], h_all.at[their_rows, :], h_send.at[0], h_recv.at[0]).wait_recv()

    wkv_copy.wait()
    kv_part[...] = lax.dot_general(h_all[:, my_depth], wkv_buf[...], (((1,), (1,)), ((), ())), preferred_element_type=f32)
    kv_stage[...] = kv_part[their_rows, :]
    kv_push = remote(kv_stage, kv_in, k_send.at[0], k_recv.at[0])
    kv_push.start()

    def cols_of(c, i):
        return pl.ds(pl.multiple_of(c * q_half + i * sub, 128), sub)

    def q_copy(i):
        return remote(stage.at[i], q_ref.at[:, cols_of(core, i)], q_send.at[i], q_recv.at[i])

    @pl.loop(0, tiles)
    def _(i):
        slot = lax.rem(i, slots)
        w_copy(i).wait()
        prod = jnp.dot(h_all[...], w_buf[slot], preferred_element_type=f32).astype(bf16)

        @pl.when(i + slots < tiles)
        def _():
            w_copy(i + slots).start()
        low, high = prod[0:rows], prod[rows:2 * rows]
        first = core == 0
        q_ref[:, cols_of(core, i)] = jnp.where(first, low, high)
        stage[i] = jnp.where(first, high, low)
        q_copy(i).start()

    kv_push.wait_recv()
    kv_ref[...] = (kv_part[my_rows, :] + kv_in[...]).astype(bf16)
    h_push.wait_send()
    kv_push.wait_send()

    @pl.loop(0, tiles)
    def _(i):
        q_copy(i).wait_send()
        remote(stage.at[i], q_ref.at[:, cols_of(other, i)], q_send.at[i], q_recv.at[i]).wait_recv()


def paired_query(hidden, attn_norm, w_query, w_kv_down, sub=256):
    bf16, f32 = jnp.bfloat16, jnp.float32
    rows, width = hidden.shape
    q_cols = w_query.shape[1]
    kv_cols = w_kv_down.shape[1]
    tiles = q_cols // 2 // sub
    slots = min(8, tiles)
    dma = pltpu.SemaphoreType.DMA
    vmem = pl.BlockSpec(memory_space=pltpu.VMEM)
    hbm = pl.BlockSpec(memory_space=pl.ANY)
    scratch = [
        pltpu.VMEM((2 * rows, width), bf16),
        pltpu.VMEM((slots, width, sub), bf16),
        pltpu.VMEM((kv_cols, width // 2), bf16),
        pltpu.VMEM((tiles, rows, sub), bf16),
        pltpu.VMEM((2 * rows, kv_cols), f32),
        pltpu.VMEM((rows, kv_cols), f32),
        pltpu.VMEM((rows, kv_cols), f32),
        dma((slots,)), dma((1,)), dma((1,)), dma((1,)), dma((1,)), dma((1,)), dma((tiles,)), dma((tiles,)),
    ]
    return pl.pallas_call(
        functools.partial(query_kernel, sub),
        out_shape=(jax.ShapeDtypeStruct((rows, q_cols), bf16), jax.ShapeDtypeStruct((rows, kv_cols), bf16)),
        in_specs=[vmem, vmem, hbm, hbm],
        out_specs=(vmem, vmem),
        scratch_shapes=scratch,
        compiler_params=pltpu.CompilerParams(collective_id=1, has_side_effects=True, vmem_limit_bytes=60_000_000),
        name='query',
    )(hidden, attn_norm, w_query, w_kv_down.T)


def tail_kernel(n, tile, sub, o_ref, x_ref, gain_ref, wo_hbm, wg_hbm, wu_hbm, wd_hbm, out_ref,
                o_all, x_half, gain_s, wo_buf, wgu_buf, x1_all, xg, acc, ssq, act_all, wd_all, part,
                stage_up, stage_dn, ring_up, ring_dn, stage_out,
                pre_send, pre_recv, wo_sem, wgu_sem, wd_sem, wdp_send, wdp_recv,
                g_send, g_recv, p_send, p_recv, a_send, a_recv, r_send, r_recv, f_send, f_recv):
    f32, bf16 = jnp.float32, jnp.bfloat16
    rows, width = x_ref.shape
    half = width // 2
    tiles = half // tile
    subs = tile // sub
    ffn = wg_hbm.shape[1]
    chips = n // 2
    reach_max = chips // 2
    chip_rows = 2 * rows
    depth = part.shape[0]

    me = lax.axis_index('tp')
    core = lax.rem(me, 2)
    chip = lax.div(me, 2)
    other = 1 - core
    partner = me + 1 - 2 * core
    upper = lax.rem(me + 2, n)
    lower = lax.rem(me + n - 2, n)
    mine = pl.multiple_of(core * half, 128)
    theirs = pl.multiple_of(other * half, 128)

    def remote(src, dst, send_sem, recv_sem, dev):
        return pltpu.make_async_remote_copy(src_ref=src, dst_ref=dst, send_sem=send_sem, recv_sem=recv_sem, device_id={'tp': dev}, device_id_type=MESH)

    def wo_copy(i):
        slot = lax.rem(i, 2)
        return pltpu.make_async_copy(wo_hbm.at[:, pl.ds(pl.multiple_of(mine + i * sub, 128), sub)], wo_buf.at[slot], wo_sem.at[slot])

    def wgu_copies(t):
        slot = lax.rem(t, 2)
        out = []
        for h in range(2):
            for k, src in enumerate((wg_hbm, wu_hbm)):
                out.append(pltpu.make_async_copy(src.at[pl.ds(pl.multiple_of(h * half + t * tile, 128), tile), :], wgu_buf.at[slot, pl.ds(h * tile, tile), pl.ds(k * ffn, ffn)], wgu_sem.at[slot, 2 * h + k]))
        return out

    def wd_copy(t):
        return pltpu.make_async_copy(wd_hbm.at[:, pl.ds(pl.multiple_of(mine + t * tile, 128), tile)], wd_all.at[t, pl.ds(pl.multiple_of(core * ffn, 128), ffn), :], wd_sem.at[t])

    def wd_push(t):
        return remote(wd_hbm.at[:, pl.ds(pl.multiple_of(theirs + t * tile, 128), tile)], wd_all.at[t, pl.ds(pl.multiple_of(core * ffn, 128), ffn), :], wdp_send.at[t], wdp_recv.at[t], partner)

    def wd_arrival(t):
        return remote(wd_hbm.at[:, pl.ds(0, tile)], wd_all.at[t, pl.ds(pl.multiple_of(other * ffn, 128), ffn), :], wdp_send.at[t], wdp_recv.at[t], partner)

    wo_copy(0).start()
    wo_copy(1).start()

    barrier = pltpu.get_barrier_semaphore()
    for dev in (partner, upper, lower):
        pl.semaphore_signal(barrier, inc=1, device_id={'tp': dev}, device_id_type=MESH)
    pl.semaphore_wait(barrier, 3)

    my_rows = pl.ds(pl.multiple_of(core * rows, rows), rows)
    their_rows = pl.ds(pl.multiple_of(other * rows, rows), rows)
    o_push = remote(o_ref, o_all.at[my_rows, :], pre_send.at[0], pre_recv.at[0], partner)
    x_push = remote(x_ref.at[:, pl.ds(theirs, half)], x_half.at[my_rows, :], pre_send.at[1], pre_recv.at[1], partner)
    o_push.start()
    x_push.start()
    o_all[my_rows, :] = o_ref[...]
    x_half[my_rows, :] = x_ref[:, pl.ds(mine, half)]
    gain = gain_ref[...].astype(f32)[None, :]
    gain_top = jnp.maximum(jnp.max(jnp.abs(gain), axis=1, keepdims=True), 1e-30)
    gain_s[...] = gain / gain_top
    acc[...] = jnp.zeros_like(acc)
    ssq[...] = jnp.zeros_like(ssq)
    remote(o_ref, o_all.at[their_rows, :], pre_send.at[0], pre_recv.at[0], partner).wait_recv()
    remote(x_ref.at[:, pl.ds(theirs, half)], x_half.at[their_rows, :], pre_send.at[1], pre_recv.at[1], partner).wait_recv()

    def reach(t, d):
        first = reach_max - lax.rem(t, 2)
        return first if d == 0 else chips - 1 - first

    def origin(h, d):
        return lax.rem(chip + chips - h, chips) if d == 0 else lax.rem(chip + h, chips)

    def block(t, src):
        return x1_all.at[core * tiles + t, pl.ds(pl.multiple_of(src * chip_rows, chip_rows), chip_rows), :]

    def ring_copy(t, src, hop, d):
        return remote(block(t, src), block(t, src), g_send.at[d, t, hop - 1], g_recv.at[d, t, hop - 1], upper if d == 0 else lower)

    def pair_copy(t, src):
        return remote(block(t, src), block(t, src), p_send.at[t], p_recv.at[t], partner)

    def produce(t):
        for q in range(subs):
            i = t * subs + q
            slot = lax.rem(i, 2)
            wo_copy(i).wait()
            prod = jnp.dot(o_all[...], wo_buf[slot], preferred_element_type=f32)
            x1 = (x_half[:, pl.ds(pl.multiple_of(i * sub, 128), sub)].astype(f32) + prod).astype(bf16)
            x1_all[core * tiles + t, pl.ds(pl.multiple_of(chip * chip_rows, chip_rows), chip_rows), pl.ds(q * sub, sub)] = x1

            @pl.when(i + 2 < tiles * subs)
            def _():
                wo_copy(i + 2).start()
        for d in range(2):
            ring_copy(t, chip, 1, d).start()
        pair_copy(t, chip).start()

    def forward(t, h):
        for d in range(2):
            @pl.when(h <= reach(t, d))
            def _():
                src = origin(h, d)
                ring_copy(t, src, h, d).wait_recv()

                @pl.when(h < reach(t, d))
                def _():
                    ring_copy(t, src, h + 1, d).start()
                pair_copy(t, src).start()

    def consume(t):
        slot = lax.rem(t, 2)
        whole = x1_all.at[other * tiles + t]
        remote(whole, whole, p_send.at[t], p_recv.at[t], partner).wait_recv()
        for h in range(2):
            @pl.loop(0, chips)
            def _(b):
                rs = pl.ds(pl.multiple_of(b * chip_rows, chip_rows), chip_rows)
                vals = x1_all[h * tiles + t, rs, :].astype(f32)
                sq = vals * vals
                tot = sq[:, 0:128]
                for k in range(1, tile // 128):
                    tot += sq[:, k * 128:(k + 1) * 128]
                ssq[rs, :] += tot
                xg[rs, h * tile:(h + 1) * tile] = (vals * gain_s[:, pl.ds(pl.multiple_of(h * half + t * tile, 128), tile)]).astype(bf16)
        for copy in wgu_copies(t):
            copy.wait()

        @pl.loop(0, 2 * ffn // 256)
        def _(i):
            cs = pl.ds(pl.multiple_of(i * 256, 256), 256)
            acc[:, cs] += jnp.dot(xg[...], wgu_buf[slot, :, cs], preferred_element_type=f32)

    last_hop = GATHER_LAG * reach_max

    def gather_round(j, carry):
        @pl.when(j < tiles)
        def _():
            produce(j)
        for h in range(1, reach_max + 1):
            t = j - GATHER_LAG * h

            @pl.when((t >= 0) & (t < tiles))
            def _():
                forward(t, h)
        t_use = j - last_hop - 1

        @pl.when((t_use >= 0) & (t_use < tiles))
        def _():
            consume(t_use)
        t_next = j - last_hop + 1

        @pl.when((t_next >= 0) & (t_next < tiles))
        def _():
            for copy in wgu_copies(t_next):
                copy.start()

        @pl.when((t_next >= 0) & (t_next < tiles))
        def _():
            wd_copy(t_next).start()
            wd_push(t_next).start()
        return carry

    lax.fori_loop(0, tiles + last_hop + 1, gather_round, 0)

    act_mine = pl.ds(pl.multiple_of(core * ffn, 128), ffn)
    act_theirs = pl.ds(pl.multiple_of(other * ffn, 128), ffn)

    def act_copy(b):
        ref = act_all.at[pl.ds(pl.multiple_of(b * chip_rows, chip_rows), chip_rows), act_mine]
        return remote(ref, ref, a_send.at[b], a_recv.at[b], partner)

    def act_arrival(b):
        ref = act_all.at[pl.ds(pl.multiple_of(b * chip_rows, chip_rows), chip_rows), act_theirs]
        return remote(ref, ref, a_send.at[b], a_recv.at[b], partner)

    @pl.loop(0, chips)
    def _(b):
        rs = pl.ds(pl.multiple_of(b * chip_rows, chip_rows), chip_rows)
        inv = lax.rsqrt(jnp.sum(ssq[rs, :], axis=1, keepdims=True) / width + EPS)
        gate = acc[rs, 0:ffn] * inv * gain_top
        upv = acc[rs, ffn:2 * ffn] * inv * gain_top
        act_all[rs, act_mine] = (gate / (1.0 + jnp.exp(-gate)) * upv).astype(bf16)
        act_copy(b).start()

    @pl.loop(0, chips)
    def _(b):
        act_arrival(b).wait_recv()

    ring_bufs = (ring_up, ring_dn)
    stage_bufs = (stage_up, stage_dn)

    def rows_of(c):
        return pl.ds(pl.multiple_of(c * chip_rows, chip_rows), chip_rows)

    def sum_copy(t, s, d):
        src = stage_bufs[d].at[t] if s == 1 else ring_bufs[d].at[t, s - 2]
        return remote(src, ring_bufs[d].at[t, s - 1], r_send.at[d, t, s - 1], r_recv.at[d, t, s - 1], upper if d == 0 else lower)

    def target(t, s, d):
        ahead = reach(t, d) - s + 1
        return lax.rem(chip + ahead, chips) if d == 0 else lax.rem(chip + chips - ahead, chips)

    def out_copy(t):
        return remote(stage_out.at[t], out_ref.at[:, pl.ds(pl.multiple_of(mine + t * tile, 128), tile)], f_send.at[t], f_recv.at[t], partner)

    def out_arrival(t):
        return remote(stage_out.at[t], out_ref.at[:, pl.ds(pl.multiple_of(theirs + t * tile, 128), tile)], f_send.at[t], f_recv.at[t], partner)

    def finish(t):
        slot = lax.rem(t, depth)
        for d in range(2):
            for s in range(1, reach_max + 1):
                @pl.when(s == reach(t, d))
                def _():
                    sum_copy(t, s, d).wait_recv()

        def total(c):
            near = pl.ds(pl.multiple_of(c * rows, rows), rows)
            far = pl.ds(pl.multiple_of(chip * chip_rows + c * rows, rows), rows)
            val = part[slot, far, :]
            for d in range(2):
                val += ring_bufs[d][t, reach(t, d) - 1, near, :].astype(f32)
            return (x1_all[core * tiles + t, far, :].astype(f32) + val).astype(bf16)

        stage_out[t] = total(other)
        out_copy(t).start()
        out_ref[:, pl.ds(pl.multiple_of(mine + t * tile, 128), tile)] = total(core)

    def scatter_round(j, carry):
        @pl.when(j < tiles)
        def _():
            slot = lax.rem(j, depth)
            wd_copy(j).wait()
            wd_arrival(j).wait_recv()

            @pl.loop(0, tile // 256)
            def _(i):
                cs = pl.ds(pl.multiple_of(i * 256, 256), 256)
                part[slot, :, cs] = jnp.dot(act_all[...], wd_all[j, :, cs], preferred_element_type=f32)
            for d in range(2):
                stage_bufs[d][j] = part[slot, rows_of(target(j, 1, d)), :].astype(bf16)
                sum_copy(j, 1, d).start()
        for s in range(2, reach_max + 1):
            t = j - SCATTER_LAG * (s - 1)

            @pl.when((t >= 0) & (t < tiles))
            def _():
                for d in range(2):
                    @pl.when(s <= reach(t, d))
                    def _():
                        sum_copy(t, s - 1, d).wait_recv()
                        buf = ring_bufs[d]
                        own = part[lax.rem(t, depth), rows_of(target(t, s, d)), :]
                        buf[t, s - 2] = (buf[t, s - 2].astype(f32) + own).astype(bf16)
                        sum_copy(t, s, d).start()
        t_end = j - SCATTER_LAG * reach_max

        @pl.when((t_end >= 0) & (t_end < tiles))
        def _():
            finish(t_end)
        return carry

    lax.fori_loop(0, tiles + SCATTER_LAG * reach_max, scatter_round, 0)

    o_push.wait_send()
    x_push.wait_send()

    @pl.loop(0, chips)
    def _(b):
        act_copy(b).wait_send()

    @pl.loop(0, tiles)
    def _(t):
        out_arrival(t).wait_recv()
        out_copy(t).wait_send()
        wd_push(t).wait_send()
        whole = x1_all.at[core * tiles + t]
        remote(whole, whole, p_send.at[t], p_recv.at[t], partner).wait_send()
        for d in range(2):
            for h in range(1, reach_max + 1):
                @pl.when(h <= reach(t, d))
                def _():
                    ring_copy(t, chip, h, d).wait_send()
                    sum_copy(t, h, d).wait_send()


def fused_tail(n, head_out, hidden, mlp_norm, w_out, w_gate, w_up, w_down, tile=512, sub=256):
    bf16, f32 = jnp.bfloat16, jnp.float32
    rows, width = hidden.shape
    inner = head_out.shape[1]
    ffn = w_gate.shape[1]
    half = width // 2
    tiles = half // tile
    chips = n // 2
    reach = chips // 2
    group = rows * n
    depth = min(tiles, SCATTER_LAG * reach + 1)
    dma = pltpu.SemaphoreType.DMA
    vmem = pl.BlockSpec(memory_space=pltpu.VMEM)
    hbm = pl.BlockSpec(memory_space=pl.ANY)
    scratch = [
        pltpu.VMEM((2 * rows, inner), bf16),
        pltpu.VMEM((2 * rows, half), bf16),
        pltpu.VMEM((1, width), f32),
        pltpu.VMEM((2, inner, sub), bf16),
        pltpu.VMEM((2, 2 * tile, 2 * ffn), bf16),
        pltpu.VMEM((2 * tiles, group, tile), bf16),
        pltpu.VMEM((group, 2 * tile), bf16),
        pltpu.VMEM((group, 2 * ffn), f32),
        pltpu.VMEM((group, 128), f32),
        pltpu.VMEM((group, 2 * ffn), bf16),
        pltpu.VMEM((tiles, 2 * ffn, tile), bf16),
        pltpu.VMEM((depth, group, tile), f32),
        pltpu.VMEM((tiles, 2 * rows, tile), bf16),
        pltpu.VMEM((tiles, 2 * rows, tile), bf16),
        pltpu.VMEM((tiles, reach, 2 * rows, tile), bf16),
        pltpu.VMEM((tiles, reach, 2 * rows, tile), bf16),
        pltpu.VMEM((tiles, rows, tile), bf16),
        dma((2,)), dma((2,)), dma((2,)), dma((2, 4)), dma((tiles,)), dma((tiles,)), dma((tiles,)),
        dma((2, tiles, reach)), dma((2, tiles, reach)), dma((tiles,)), dma((tiles,)),
        dma((chips,)), dma((chips,)), dma((2, tiles, reach)), dma((2, tiles, reach)), dma((tiles,)), dma((tiles,)),
    ]
    return pl.pallas_call(
        functools.partial(tail_kernel, n, tile, sub),
        out_shape=jax.ShapeDtypeStruct((rows, width), bf16),
        in_specs=[vmem, vmem, vmem, hbm, hbm, hbm, hbm],
        out_specs=vmem,
        scratch_shapes=scratch,
        compiler_params=pltpu.CompilerParams(collective_id=0, has_side_effects=True, vmem_limit_bytes=67_043_328),
        name='tail',
    )(head_out, hidden, mlp_norm, w_out, w_gate, w_up, w_down)


def solution(mesh):
    rows_spec = P(('dp', 'tp'), None)
    cache_spec = P(('dp', 'tp'), None, None)
    whole = P()
    in_specs = (rows_spec, cache_spec, cache_spec, P(('dp', 'tp')), whole, whole, whole, whole, whole, whole, whole, whole, P(None, 'tp'), P(None, 'tp'), P('tp', None))
    out_specs = (rows_spec, rows_spec, rows_spec)

    def device_step(hidden, cache_lat, cache_rope, seq_lens, attn_norm, w_query, w_kv_down, kv_norm, w_key_up, w_val_up, w_out, mlp_norm, w_gate, w_up, w_down):
        head_out, lat_new, rope_new = attention_block(hidden, cache_lat, cache_rope, seq_lens, attn_norm, w_query, w_kv_down, kv_norm, w_key_up, w_val_up)
        out_hidden = fused_tail(mesh.shape['tp'], head_out, hidden, mlp_norm, w_out, w_gate, w_up, w_down)
        return out_hidden, lat_new, rope_new

    return jax.shard_map(device_step, mesh=mesh, in_specs=in_specs, out_specs=out_specs, check_vma=False)
```

```python
import functools

import jax
import jax.numpy as jnp
from jax import lax
from jax.experimental import pallas as pl
from jax.experimental.pallas import tpu as pltpu
from jax.sharding import PartitionSpec as P

EPS = 1e-6
ROPE_BASE = 10000.0
value_a7 = 512
ROPE_DIM = 64
NOPE_DIM = 128
SCALE = (NOPE_DIM + ROPE_DIM) ** -0.5


def rms_norm(vals, gain):
    vals32 = vals.astype(jnp.float32)
    inv_rms = lax.rsqrt(jnp.mean(vals32 * vals32, axis=-1, keepdims=True) + EPS)
    return (vals32 * inv_rms * gain.astype(jnp.float32)).astype(jnp.bfloat16)


def rotate(vals, cos_tab, sin_tab):
    half = vals.shape[-1] // 2
    first = vals[..., :half]
    second = vals[..., half:]
    return jnp.concatenate([first * cos_tab - second * sin_tab, second * cos_tab + first * sin_tab], axis=-1)


def rope_tables(seq_lens):
    inv_freq = ROPE_BASE ** (-jnp.arange(0, ROPE_DIM, 2, dtype=jnp.float32) / ROPE_DIM)
    angles = seq_lens.astype(jnp.float32)[:, None] * inv_freq[None, :]
    return jnp.cos(angles), jnp.sin(angles)


def attention_block(hidden, cache_lat, cache_rope, seq_lens, attn_norm, w_query, w_kv_down, kv_norm, w_key_up, w_val_up):
    rows = hidden.shape[0]
    heads = w_key_up.shape[1] // NOPE_DIM
    query, kv_proj = paired_query(hidden, attn_norm, w_query, w_kv_down)
    query = query.reshape(rows, heads, NOPE_DIM + ROPE_DIM)
    lat_new = rms_norm(kv_proj[:, :value_a7], kv_norm)
    cos_tab, sin_tab = rope_tables(seq_lens)
    rope_new = rotate(kv_proj[:, value_a7:].astype(jnp.float32), cos_tab, sin_tab).astype(jnp.bfloat16)
    q_rot = rotate(query[:, :, NOPE_DIM:].astype(jnp.float32), cos_tab[:, None, :], sin_tab[:, None, :]).astype(jnp.bfloat16)
    key_up = w_key_up.reshape(value_a7, heads, NOPE_DIM)
    q_lat = jnp.einsum('bhn,khn->bhk', query[:, :, :NOPE_DIM], key_up, preferred_element_type=jnp.float32).astype(jnp.bfloat16)
    scores = (jnp.einsum('bhk,bsk->bhs', q_lat, cache_lat, preferred_element_type=jnp.float32) + jnp.einsum('bhr,bsr->bhs', q_rot, cache_rope, preferred_element_type=jnp.float32)) * SCALE
    score_new = (jnp.einsum('bhk,bk->bh', q_lat, lat_new, preferred_element_type=jnp.float32) + jnp.einsum('bhr,br->bh', q_rot, rope_new, preferred_element_type=jnp.float32)) * SCALE
    slots = cache_lat.shape[1]
    valid = jnp.arange(slots)[None, None, :] < seq_lens[:, None, None]
    scores = jnp.where(valid, scores, -jnp.inf)
    top = jnp.maximum(jnp.max(scores, axis=-1), score_new)
    expo = jnp.exp(scores - top[..., None])
    expo_new = jnp.exp(score_new - top)
    denom = jnp.sum(expo, axis=-1) + expo_new
    probs = (expo / denom[..., None]).astype(jnp.bfloat16)
    prob_new = (expo_new / denom).astype(jnp.bfloat16)
    lat_sum = jnp.einsum('bhs,bsk->bhk', probs, cache_lat, preferred_element_type=jnp.float32) + prob_new.astype(jnp.float32)[..., None] * lat_new.astype(jnp.float32)[:, None, :]
    head_out = head_values(lat_sum, w_val_up)
    return head_out, lat_new, rope_new

MESH = pl.DeviceIdType.MESH
GATHER_LAG = 1
SCATTER_LAG = 2

def head_kernel(heads, lat_ref, val_ref, out_ref, lat_buf):
    rows = out_ref.shape[0]
    width = val_ref.shape[1]
    dim = width // heads
    lanes, total, _ = lat_buf.shape
    quad, group = 4, 16
    step = total // 16

    @pl.loop(0, 16)
    def _(b):
        rs = pl.ds(pl.multiple_of(b * step, step), step)
        for i in range(lanes):
            lat_buf[i, rs, :] = lat_ref[rs, i * 128:(i + 1) * 128]

    @pl.loop(0, heads // group)
    def _(c):
        for g in range(group // quad):
            first = c * group + g * quad
            parts = [jnp.concatenate([lat_buf[i, pl.ds(first + k, rows, stride=heads), :] for k in range(quad)], axis=0) for i in range(lanes)]
            lhs = jnp.concatenate(parts, axis=1).astype(jnp.bfloat16)
            cols = pl.ds(pl.multiple_of(first * dim, quad * dim), quad * dim)
            prod = jnp.dot(lhs, val_ref[:, cols], preferred_element_type=jnp.float32)
            diag = [prod[k * rows:(k + 1) * rows, k * dim:(k + 1) * dim] for k in range(quad)]
            out_ref[:, cols] = jnp.concatenate(diag, axis=1).astype(jnp.bfloat16)


def head_values(lat_sum, w_val_up):
    rows, heads, depth = lat_sum.shape
    width = w_val_up.shape[1]
    vmem = pl.BlockSpec(memory_space=pltpu.VMEM)
    return pl.pallas_call(
        functools.partial(head_kernel, heads),
        out_shape=jax.ShapeDtypeStruct((rows, width), jnp.bfloat16),
        in_specs=[vmem, vmem],
        out_specs=vmem,
        scratch_shapes=[pltpu.VMEM((depth // 128, rows * heads, 128), jnp.float32)],
        cost_estimate=pl.CostEstimate(flops=2 * rows * depth * width, bytes_accessed=2 * depth * width, transcendentals=0),
        compiler_params=pltpu.CompilerParams(vmem_limit_bytes=24_000_000),
        name='head_values',
    )(lat_sum.reshape(rows * heads, depth), w_val_up)


def query_kernel(sub, x_ref, gain_ref, wq_hbm, wkv_hbm, q_ref, kv_ref,
                 h_all, w_buf, wkv_buf, stage, kv_part, kv_stage, kv_in,
                 w_sem, wkv_sem, h_send, h_recv, k_send, k_recv, q_send, q_recv):
    f32, bf16 = jnp.float32, jnp.bfloat16
    rows, width = x_ref.shape
    half = width // 2
    q_half = wq_hbm.shape[1] // 2
    tiles = q_half // sub
    slots = w_buf.shape[0]
    me = lax.axis_index('tp')
    core = lax.rem(me, 2)
    other = 1 - core
    partner = me + 1 - 2 * core
    my_rows = pl.ds(pl.multiple_of(core * rows, rows), rows)
    their_rows = pl.ds(pl.multiple_of(other * rows, rows), rows)
    my_depth = pl.ds(pl.multiple_of(core * half, 128), half)

    def remote(src, dst, send_sem, recv_sem):
        return pltpu.make_async_remote_copy(src_ref=src, dst_ref=dst, send_sem=send_sem, recv_sem=recv_sem, device_id={'tp': partner}, device_id_type=MESH)

    def w_copy(i):
        slot = lax.rem(i, slots)
        return pltpu.make_async_copy(wq_hbm.at[:, pl.ds(pl.multiple_of(core * q_half + i * sub, 128), sub)], w_buf.at[slot], w_sem.at[slot])

    wkv_copy = pltpu.make_async_copy(wkv_hbm.at[:, my_depth], wkv_buf, wkv_sem.at[0])
    wkv_copy.start()
    for i in range(slots):
        w_copy(i).start()

    barrier = pltpu.get_barrier_semaphore()
    pl.semaphore_signal(barrier, inc=1, device_id={'tp': partner}, device_id_type=MESH)

    step = min(1024, width)
    tot = jnp.zeros((rows, 128), f32)
    for c in range(0, width, step):
        vals = x_ref[:, c:c + step].astype(f32)
        sq = vals * vals
        for k in range(0, step, 128):
            tot += sq[:, k:k + 128]
    inv = lax.rsqrt(jnp.sum(tot, axis=1, keepdims=True) / width + EPS)
    for c in range(0, width, step):
        vals = x_ref[:, c:c + step].astype(f32)
        h_all[my_rows, c:c + step] = (vals * inv * gain_ref[c:c + step].astype(f32)[None, :]).astype(bf16)

    pl.semaphore_wait(barrier, 1)
    h_push = remote(h_all.at[my_rows, :], h_all.at[my_rows, :], h_send.at[0], h_recv.at[0])
    h_push.start()
    remote(h_all.at[their_rows, :], h_all.at[their_rows, :], h_send.at[0], h_recv.at[0]).wait_recv()

    wkv_copy.wait()
    kv_part[...] = lax.dot_general(h_all[:, my_depth], wkv_buf[...], (((1,), (1,)), ((), ())), preferred_element_type=f32)
    kv_stage[...] = kv_part[their_rows, :]
    kv_push = remote(kv_stage, kv_in, k_send.at[0], k_recv.at[0])
    kv_push.start()

    def cols_of(c, i):
        return pl.ds(pl.multiple_of(c * q_half + i * sub, 128), sub)

    def q_copy(i):
        return remote(stage.at[i], q_ref.at[:, cols_of(core, i)], q_send.at[i], q_recv.at[i])

    @pl.loop(0, tiles)
    def _(i):
        slot = lax.rem(i, slots)
        w_copy(i).wait()
        prod = jnp.dot(h_all[...], w_buf[slot], preferred_element_type=f32).astype(bf16)

        @pl.when(i + slots < tiles)
        def _():
            w_copy(i + slots).start()
        low, high = prod[0:rows], prod[rows:2 * rows]
        first = core == 0
        q_ref[:, cols_of(core, i)] = jnp.where(first, low, high)
        stage[i] = jnp.where(first, high, low)
        q_copy(i).start()

    kv_push.wait_recv()
    kv_ref[...] = (kv_part[my_rows, :] + kv_in[...]).astype(bf16)
    h_push.wait_send()
    kv_push.wait_send()

    @pl.loop(0, tiles)
    def _(i):
        q_copy(i).wait_send()
        remote(stage.at[i], q_ref.at[:, cols_of(other, i)], q_send.at[i], q_recv.at[i]).wait_recv()


def paired_query(hidden, attn_norm, w_query, w_kv_down, sub=256):
    bf16, f32 = jnp.bfloat16, jnp.float32
    rows, width = hidden.shape
    q_cols = w_query.shape[1]
    kv_cols = w_kv_down.shape[1]
    tiles = q_cols // 2 // sub
    slots = min(8, tiles)
    dma = pltpu.SemaphoreType.DMA
    vmem = pl.BlockSpec(memory_space=pltpu.VMEM)
    hbm = pl.BlockSpec(memory_space=pl.ANY)
    scratch = [
        pltpu.VMEM((2 * rows, width), bf16),
        pltpu.VMEM((slots, width, sub), bf16),
        pltpu.VMEM((kv_cols, width // 2), bf16),
        pltpu.VMEM((tiles, rows, sub), bf16),
        pltpu.VMEM((2 * rows, kv_cols), f32),
        pltpu.VMEM((rows, kv_cols), f32),
        pltpu.VMEM((rows, kv_cols), f32),
        dma((slots,)), dma((1,)), dma((1,)), dma((1,)), dma((1,)), dma((1,)), dma((tiles,)), dma((tiles,)),
    ]
    return pl.pallas_call(
        functools.partial(query_kernel, sub),
        out_shape=(jax.ShapeDtypeStruct((rows, q_cols), bf16), jax.ShapeDtypeStruct((rows, kv_cols), bf16)),
        in_specs=[vmem, vmem, hbm, hbm],
        out_specs=(vmem, vmem),
        scratch_shapes=scratch,
        compiler_params=pltpu.CompilerParams(collective_id=1, has_side_effects=True, vmem_limit_bytes=60_000_000),
        name='query',
    )(hidden, attn_norm, w_query, w_kv_down.T)


def tail_kernel(n, tile, sub, o_ref, x_ref, gain_ref, wo_hbm, wg_hbm, wu_hbm, wd_hbm, out_ref,
                o_all, x_half, gain_s, wo_buf, wgu_buf, x1_all, xg, acc, ssq, act_all, wd_all, part,
                stage_up, stage_dn, ring_up, ring_dn, stage_out,
                pre_send, pre_recv, wo_sem, wgu_sem, wd_sem, wdp_send, wdp_recv,
                g_send, g_recv, p_send, p_recv, a_send, a_recv, r_send, r_recv, f_send, f_recv):
    f32, bf16 = jnp.float32, jnp.bfloat16
    rows, width = x_ref.shape
    half = width // 2
    tiles = half // tile
    subs = tile // sub
    ffn = wg_hbm.shape[1]
    chips = n // 2
    reach_max = chips // 2
    chip_rows = 2 * rows
    depth = part.shape[0]

    me = lax.axis_index('tp')
    core = lax.rem(me, 2)
    chip = lax.div(me, 2)
    other = 1 - core
    partner = me + 1 - 2 * core
    upper = lax.rem(me + 2, n)
    lower = lax.rem(me + n - 2, n)
    mine = pl.multiple_of(core * half, 128)
    theirs = pl.multiple_of(other * half, 128)

    def remote(src, dst, send_sem, recv_sem, dev):
        return pltpu.make_async_remote_copy(src_ref=src, dst_ref=dst, send_sem=send_sem, recv_sem=recv_sem, device_id={'tp': dev}, device_id_type=MESH)

    def wo_copy(i):
        slot = lax.rem(i, 2)
        return pltpu.make_async_copy(wo_hbm.at[:, pl.ds(pl.multiple_of(mine + i * sub, 128), sub)], wo_buf.at[slot], wo_sem.at[slot])

    def wgu_copies(t):
        slot = lax.rem(t, 2)
        out = []
        for h in range(2):
            for k, src in enumerate((wg_hbm, wu_hbm)):
                out.append(pltpu.make_async_copy(src.at[pl.ds(pl.multiple_of(h * half + t * tile, 128), tile), :], wgu_buf.at[slot, pl.ds(h * tile, tile), pl.ds(k * ffn, ffn)], wgu_sem.at[slot, 2 * h + k]))
        return out

    def wd_copy(t):
        return pltpu.make_async_copy(wd_hbm.at[:, pl.ds(pl.multiple_of(mine + t * tile, 128), tile)], wd_all.at[t, pl.ds(pl.multiple_of(core * ffn, 128), ffn), :], wd_sem.at[t])

    def wd_push(t):
        return remote(wd_hbm.at[:, pl.ds(pl.multiple_of(theirs + t * tile, 128), tile)], wd_all.at[t, pl.ds(pl.multiple_of(core * ffn, 128), ffn), :], wdp_send.at[t], wdp_recv.at[t], partner)

    def wd_arrival(t):
        return remote(wd_hbm.at[:, pl.ds(0, tile)], wd_all.at[t, pl.ds(pl.multiple_of(other * ffn, 128), ffn), :], wdp_send.at[t], wdp_recv.at[t], partner)

    wo_copy(0).start()
    wo_copy(1).start()

    barrier = pltpu.get_barrier_semaphore()
    for dev in (partner, upper, lower):
        pl.semaphore_signal(barrier, inc=1, device_id={'tp': dev}, device_id_type=MESH)
    pl.semaphore_wait(barrier, 3)

    my_rows = pl.ds(pl.multiple_of(core * rows, rows), rows)
    their_rows = pl.ds(pl.multiple_of(other * rows, rows), rows)
    o_push = remote(o_ref, o_all.at[my_rows, :], pre_send.at[0], pre_recv.at[0], partner)
    x_push = remote(x_ref.at[:, pl.ds(theirs, half)], x_half.at[my_rows, :], pre_send.at[1], pre_recv.at[1], partner)
    o_push.start()
    x_push.start()
    o_all[my_rows, :] = o_ref[...]
    x_half[my_rows, :] = x_ref[:, pl.ds(mine, half)]
    gain = gain_ref[...].astype(f32)[None, :]
    gain_top = jnp.maximum(jnp.max(jnp.abs(gain), axis=1, keepdims=True), 1e-30)
    gain_s[...] = gain / gain_top
    acc[...] = jnp.zeros_like(acc)
    ssq[...] = jnp.zeros_like(ssq)
    remote(o_ref, o_all.at[their_rows, :], pre_send.at[0], pre_recv.at[0], partner).wait_recv()
    remote(x_ref.at[:, pl.ds(theirs, half)], x_half.at[their_rows, :], pre_send.at[1], pre_recv.at[1], partner).wait_recv()

    def reach(t, d):
        first = reach_max - lax.rem(t, 2)
        return first if d == 0 else chips - 1 - first

    def origin(h, d):
        return lax.rem(chip + chips - h, chips) if d == 0 else lax.rem(chip + h, chips)

    def block(t, src):
        return x1_all.at[core * tiles + t, pl.ds(pl.multiple_of(src * chip_rows, chip_rows), chip_rows), :]

    def ring_copy(t, src, hop, d):
        return remote(block(t, src), block(t, src), g_send.at[d, t, hop - 1], g_recv.at[d, t, hop - 1], upper if d == 0 else lower)

    def pair_copy(t, src):
        return remote(block(t, src), block(t, src), p_send.at[t], p_recv.at[t], partner)

    def produce(t):
        for q in range(subs):
            i = t * subs + q
            slot = lax.rem(i, 2)
            wo_copy(i).wait()
            prod = jnp.dot(o_all[...], wo_buf[slot], preferred_element_type=f32)
            x1 = (x_half[:, pl.ds(pl.multiple_of(i * sub, 128), sub)].astype(f32) + prod).astype(bf16)
            x1_all[core * tiles + t, pl.ds(pl.multiple_of(chip * chip_rows, chip_rows), chip_rows), pl.ds(q * sub, sub)] = x1

            @pl.when(i + 2 < tiles * subs)
            def _():
                wo_copy(i + 2).start()
        for d in range(2):
            ring_copy(t, chip, 1, d).start()
        pair_copy(t, chip).start()

    def forward(t, h):
        for d in range(2):
            @pl.when(h <= reach(t, d))
            def _():
                src = origin(h, d)
                ring_copy(t, src, h, d).wait_recv()

                @pl.when(h < reach(t, d))
                def _():
                    ring_copy(t, src, h + 1, d).start()
                pair_copy(t, src).start()

    def consume(t):
        slot = lax.rem(t, 2)
        whole = x1_all.at[other * tiles + t]
        remote(whole, whole, p_send.at[t], p_recv.at[t], partner).wait_recv()
        for h in range(2):
            @pl.loop(0, chips)
            def _(b):
                rs = pl.ds(pl.multiple_of(b * chip_rows, chip_rows), chip_rows)
                vals = x1_all[h * tiles + t, rs, :].astype(f32)
                sq = vals * vals
                tot = sq[:, 0:128]
                for k in range(1, tile // 128):
                    tot += sq[:, k * 128:(k + 1) * 128]
                ssq[rs, :] += tot
                xg[rs, h * tile:(h + 1) * tile] = (vals * gain_s[:, pl.ds(pl.multiple_of(h * half + t * tile, 128), tile)]).astype(bf16)
        for copy in wgu_copies(t):
            copy.wait()

        @pl.loop(0, 2 * ffn // 256)
        def _(i):
            cs = pl.ds(pl.multiple_of(i * 256, 256), 256)
            acc[:, cs] += jnp.dot(xg[...], wgu_buf[slot, :, cs], preferred_element_type=f32)

    last_hop = GATHER_LAG * reach_max

    def gather_round(j, carry):
        @pl.when(j < tiles)
        def _():
            produce(j)
        def forward_hops(hops):
            for h in hops:
                t = j - GATHER_LAG * h

                @pl.when((t >= 0) & (t < tiles))
                def _():
                    forward(t, h)

        t_use = j - last_hop - 1
        forward_hops(range(1, 2))

        @pl.when((t_use >= 0) & (t_use < tiles))
        def _():
            consume(t_use)
        forward_hops(range(2, reach_max + 1))
        t_next = j - last_hop + 1

        @pl.when((t_next >= 0) & (t_next < tiles))
        def _():
            for copy in wgu_copies(t_next):
                copy.start()

        @pl.when((t_next >= 0) & (t_next < tiles))
        def _():
            wd_copy(t_next).start()
            wd_push(t_next).start()
        return carry

    lax.fori_loop(0, tiles + last_hop + 1, gather_round, 0)

    act_mine = pl.ds(pl.multiple_of(core * ffn, 128), ffn)
    act_theirs = pl.ds(pl.multiple_of(other * ffn, 128), ffn)

    def act_copy(b):
        ref = act_all.at[pl.ds(pl.multiple_of(b * chip_rows, chip_rows), chip_rows), act_mine]
        return remote(ref, ref, a_send.at[b], a_recv.at[b], partner)

    def act_arrival(b):
        ref = act_all.at[pl.ds(pl.multiple_of(b * chip_rows, chip_rows), chip_rows), act_theirs]
        return remote(ref, ref, a_send.at[b], a_recv.at[b], partner)

    @pl.loop(0, chips)
    def _(b):
        rs = pl.ds(pl.multiple_of(b * chip_rows, chip_rows), chip_rows)
        inv = lax.rsqrt(jnp.sum(ssq[rs, :], axis=1, keepdims=True) / width + EPS)
        gate = acc[rs, 0:ffn] * inv * gain_top
        upv = acc[rs, ffn:2 * ffn] * inv * gain_top
        act_all[rs, act_mine] = (gate / (1.0 + jnp.exp(-gate)) * upv).astype(bf16)
        act_copy(b).start()

    @pl.loop(0, chips)
    def _(b):
        act_arrival(b).wait_recv()

    ring_bufs = (ring_up, ring_dn)
    stage_bufs = (stage_up, stage_dn)

    def rows_of(c):
        return pl.ds(pl.multiple_of(c * chip_rows, chip_rows), chip_rows)

    def sum_copy(t, s, d):
        src = stage_bufs[d].at[t] if s == 1 else ring_bufs[d].at[t, s - 2]
        return remote(src, ring_bufs[d].at[t, s - 1], r_send.at[d, t, s - 1], r_recv.at[d, t, s - 1], upper if d == 0 else lower)

    def target(t, s, d):
        ahead = reach(t, d) - s + 1
        return lax.rem(chip + ahead, chips) if d == 0 else lax.rem(chip + chips - ahead, chips)

    def out_copy(t):
        return remote(stage_out.at[t], out_ref.at[:, pl.ds(pl.multiple_of(mine + t * tile, 128), tile)], f_send.at[t], f_recv.at[t], partner)

    def out_arrival(t):
        return remote(stage_out.at[t], out_ref.at[:, pl.ds(pl.multiple_of(theirs + t * tile, 128), tile)], f_send.at[t], f_recv.at[t], partner)

    def finish(t):
        slot = lax.rem(t, depth)
        for d in range(2):
            for s in range(1, reach_max + 1):
                @pl.when(s == reach(t, d))
                def _():
                    sum_copy(t, s, d).wait_recv()

        def total(c):
            near = pl.ds(pl.multiple_of(c * rows, rows), rows)
            far = pl.ds(pl.multiple_of(chip * chip_rows + c * rows, rows), rows)
            val = part[slot, far, :]
            for d in range(2):
                val += ring_bufs[d][t, reach(t, d) - 1, near, :].astype(f32)
            return (x1_all[core * tiles + t, far, :].astype(f32) + val).astype(bf16)

        stage_out[t] = total(other)
        out_copy(t).start()
        out_ref[:, pl.ds(pl.multiple_of(mine + t * tile, 128), tile)] = total(core)

    def scatter_round(j, carry):
        @pl.when(j < tiles)
        def _():
            slot = lax.rem(j, depth)
            wd_copy(j).wait()
            wd_arrival(j).wait_recv()

            @pl.loop(0, tile // 256)
            def _(i):
                cs = pl.ds(pl.multiple_of(i * 256, 256), 256)
                part[slot, :, cs] = jnp.dot(act_all[...], wd_all[j, :, cs], preferred_element_type=f32)
            for d in range(2):
                stage_bufs[d][j] = part[slot, rows_of(target(j, 1, d)), :].astype(bf16)
                sum_copy(j, 1, d).start()
        for s in range(2, reach_max + 1):
            t = j - SCATTER_LAG * (s - 1)

            @pl.when((t >= 0) & (t < tiles))
            def _():
                for d in range(2):
                    @pl.when(s <= reach(t, d))
                    def _():
                        sum_copy(t, s - 1, d).wait_recv()
                        buf = ring_bufs[d]
                        own = part[lax.rem(t, depth), rows_of(target(t, s, d)), :]
                        buf[t, s - 2] = (buf[t, s - 2].astype(f32) + own).astype(bf16)
                        sum_copy(t, s, d).start()
        t_end = j - SCATTER_LAG * reach_max

        @pl.when((t_end >= 0) & (t_end < tiles))
        def _():
            finish(t_end)
        return carry

    lax.fori_loop(0, tiles + SCATTER_LAG * reach_max, scatter_round, 0)

    o_push.wait_send()
    x_push.wait_send()

    @pl.loop(0, chips)
    def _(b):
        act_copy(b).wait_send()

    @pl.loop(0, tiles)
    def _(t):
        out_arrival(t).wait_recv()
        out_copy(t).wait_send()
        wd_push(t).wait_send()
        whole = x1_all.at[core * tiles + t]
        remote(whole, whole, p_send.at[t], p_recv.at[t], partner).wait_send()
        for d in range(2):
            for h in range(1, reach_max + 1):
                @pl.when(h <= reach(t, d))
                def _():
                    ring_copy(t, chip, h, d).wait_send()
                    sum_copy(t, h, d).wait_send()


def fused_tail(n, head_out, hidden, mlp_norm, w_out, w_gate, w_up, w_down, tile=512, sub=256):
    bf16, f32 = jnp.bfloat16, jnp.float32
    rows, width = hidden.shape
    inner = head_out.shape[1]
    ffn = w_gate.shape[1]
    half = width // 2
    tiles = half // tile
    chips = n // 2
    reach = chips // 2
    group = rows * n
    depth = min(tiles, SCATTER_LAG * reach + 1)
    dma = pltpu.SemaphoreType.DMA
    vmem = pl.BlockSpec(memory_space=pltpu.VMEM)
    hbm = pl.BlockSpec(memory_space=pl.ANY)
    scratch = [
        pltpu.VMEM((2 * rows, inner), bf16),
        pltpu.VMEM((2 * rows, half), bf16),
        pltpu.VMEM((1, width), f32),
        pltpu.VMEM((2, inner, sub), bf16),
        pltpu.VMEM((2, 2 * tile, 2 * ffn), bf16),
        pltpu.VMEM((2 * tiles, group, tile), bf16),
        pltpu.VMEM((group, 2 * tile), bf16),
        pltpu.VMEM((group, 2 * ffn), f32),
        pltpu.VMEM((group, 128), f32),
        pltpu.VMEM((group, 2 * ffn), bf16),
        pltpu.VMEM((tiles, 2 * ffn, tile), bf16),
        pltpu.VMEM((depth, group, tile), f32),
        pltpu.VMEM((tiles, 2 * rows, tile), bf16),
        pltpu.VMEM((tiles, 2 * rows, tile), bf16),
        pltpu.VMEM((tiles, reach, 2 * rows, tile), bf16),
        pltpu.VMEM((tiles, reach, 2 * rows, tile), bf16),
        pltpu.VMEM((tiles, rows, tile), bf16),
        dma((2,)), dma((2,)), dma((2,)), dma((2, 4)), dma((tiles,)), dma((tiles,)), dma((tiles,)),
        dma((2, tiles, reach)), dma((2, tiles, reach)), dma((tiles,)), dma((tiles,)),
        dma((chips,)), dma((chips,)), dma((2, tiles, reach)), dma((2, tiles, reach)), dma((tiles,)), dma((tiles,)),
    ]
    return pl.pallas_call(
        functools.partial(tail_kernel, n, tile, sub),
        out_shape=jax.ShapeDtypeStruct((rows, width), bf16),
        in_specs=[vmem, vmem, vmem, hbm, hbm, hbm, hbm],
        out_specs=vmem,
        scratch_shapes=scratch,
        compiler_params=pltpu.CompilerParams(collective_id=0, has_side_effects=True, vmem_limit_bytes=67_043_328),
        name='tail',
    )(head_out, hidden, mlp_norm, w_out, w_gate, w_up, w_down)


def solution(mesh):
    rows_spec = P(('dp', 'tp'), None)
    cache_spec = P(('dp', 'tp'), None, None)
    whole = P()
    in_specs = (rows_spec, cache_spec, cache_spec, P(('dp', 'tp')), whole, whole, whole, whole, whole, whole, whole, whole, P(None, 'tp'), P(None, 'tp'), P('tp', None))
    out_specs = (rows_spec, rows_spec, rows_spec)

    def device_step(hidden, cache_lat, cache_rope, seq_lens, attn_norm, w_query, w_kv_down, kv_norm, w_key_up, w_val_up, w_out, mlp_norm, w_gate, w_up, w_down):
        head_out, lat_new, rope_new = attention_block(hidden, cache_lat, cache_rope, seq_lens, attn_norm, w_query, w_kv_down, kv_norm, w_key_up, w_val_up)
        out_hidden = fused_tail(mesh.shape['tp'], head_out, hidden, mlp_norm, w_out, w_gate, w_up, w_down)
        return out_hidden, lat_new, rope_new

    return jax.shard_map(device_step, mesh=mesh, in_specs=in_specs, out_specs=out_specs, check_vma=False)
```
